32 devices in a mesh: section: 4 (over y, x), fsdp: 8 (over z, core).
Axes of the slice: x: 2, y: 2, z: 4, core: 2. Of those that a mesh axis runs over, the one named last changes fastest.
Arguments:
- codes: int32 [4, 8192, 512], P('section', 'fsdp'), may hold values from 0 to 15
- scale_codes: int32 [4, 8192, 8], P('section', 'fsdp'), may hold values from 0 to 255
- second_scales: float32 [4, 256], P('section', 'fsdp'), may hold values from 0.015 to 0.09
- gains: bfloat16 [4, 8192], P('section'), may hold values from 0.5 to 1.5
- down_adapter: bfloat16 [4, 8192, 64], P('section'), may hold values from -0.0625 to 0.0625
- up_projection_weight: bfloat16 [4, 512, 64], P('section'), may hold values from -0.75 to 0.75
- hidden_in: bfloat16 [1024, 8192], P('fsdp'), may hold values from -6 to 6
- cotangent: bfloat16 [1024, 8192], P('fsdp'), may hold values from -6 to 6
Outputs:
- input_grad: bfloat16 [4, 1024, 8192], P('section', 'fsdp')
- grad_down: float32 [4, 8192, 64], P('section', 'fsdp')
- grad_up: float32 [4, 512, 64], P('section', 'fsdp')
The draws below stay inside these ranges and needn't reach their ends.
All inputs are finite; a program needn't handle non-finite values.
Results may differ from the reference program's by a relative error of at most 0.025.
Values may be sent and summed in bfloat16 or wider, within the bound.
No kernel may reach another device: no remote copies, remote signals or barrier semaphores. Data moves between devices by JAX's collectives and lax.ppermute only.
A program may use at most 128 MiB of HBM per device.

```python
import math
import jax
import jax.numpy as jnp
from jax import lax

D = 8192
HEAD = 128
GROUP = 8
KV_HEADS = 4
RANK = 64
BLOCK = 64
SROWS = 32
KVW = 512
TOKENS = 1024
LAYERS = 4


def touch_ends(result, stream_key, low, largest):
    longest = result.shape.index(max(result.shape))
    spots = []
    for shift in (0, 1):
        where = [jax.random.randint(jax.random.fold_in(stream_key, axis), (), 0, length) for axis, length in enumerate(result.shape)]
        where[longest] = (where[longest] + shift) % result.shape[longest]
        spots.append(tuple(where))
    return result.at[spots[0]].set(low).at[spots[1]].set(largest)


def with_spikes(drawn, own_key, source, target, parts, factor):
    def block_of(dim):
        return (jnp.arange(drawn.shape[dim]) // (drawn.shape[dim] // parts)).reshape((-1,) + (1,) * (drawn.ndim - 1 - dim))

    one_side = jax.random.permutation(own_key, parts)[block_of(target)]
    far = (block_of(target) + parts // 2) % parts
    return jnp.where((block_of(source) == one_side) | (block_of(source) == far), factor * drawn, drawn)


def block_scale(rng, dims, cuts, least, high):
    loudness, own = 1.0, jax.random.fold_in(rng, 6)
    for axis_at, blocks in cuts:
        draws = jnp.exp(jax.random.uniform(jax.random.fold_in(own, axis_at), (blocks,), jnp.float32, least / len(cuts), high / len(cuts)))
        loudness = loudness * jnp.repeat(draws, dims[axis_at] // blocks).reshape([-1 if axis == axis_at else 1 for axis in range(len(dims))])
    return loudness


def noise(rng, extent, scale, bound, pieces=(), kind=jnp.bfloat16):
    result = jax.random.normal(rng, extent, jnp.float32) * scale
    if len(pieces) > 0:
        result = block_scale(rng, extent, pieces, -0.22, 0.18) * result
    return jnp.clip(result, min=-bound, max=bound).astype(kind)


def bell_draw_with(rng, dims, spread, most, pieces, heavy, kind=jnp.bfloat16):
    drawn = spread * jax.random.normal(rng, dims, jnp.float32)
    if pieces:
        drawn = drawn * block_scale(rng, dims, pieces, -0.22, 0.18)
    return jnp.clip(with_spikes(drawn, jax.random.fold_in(rng, 3), *heavy), -most, most).astype(kind)


def setup_inputs(seed: int = 0) -> dict:
    splits = jax.random.split(jax.random.key(seed), 9)
    return {
        "codes": touch_ends(jax.random.randint(splits[0], (LAYERS, D, KVW), 0, 16), jax.random.fold_in(splits[0], 1), 0, 15).astype(jnp.int32),
        "scale_codes": touch_ends(jax.random.randint(splits[1], (LAYERS, D, KVW // BLOCK), 0, 256), jax.random.fold_in(splits[1], 1), 0, 255).astype(jnp.int32),
        "second_scales": jnp.clip(jnp.exp(math.log(0.09) - 1.7917595 * jax.random.uniform(splits[2], (LAYERS, D // SROWS), jnp.float32) ** block_scale(splits[2], (LAYERS, D // SROWS), ((0, 4), (1, 8)), -0.2, 0.2)), 0.015, 0.09),
        "gains": jnp.clip(1.0 + 0.1 * jax.random.normal(splits[3], (LAYERS, D), jnp.float32), 0.5, 1.5).astype(jnp.bfloat16),
        "down_adapter": noise(splits[4], (LAYERS, D, RANK), D ** -0.5, 0.0625, ((0, 4),)),
        "up_projection_weight": noise(splits[5], (LAYERS, KVW, RANK), RANK ** -0.5, 0.75, ((0, 4),)),
        "hidden_in": bell_draw_with(splits[6], (TOKENS, D), 1.0, 6.0, ((0, 8),), (0, 1, 8, 2.0)),
        "cotangent": noise(splits[7], (TOKENS, D), 1.0, 6.0, ((0, 8),)),
    }


NF4_TABLE = (-1.0, -0.6961928009986877, -0.5250730514526367, -0.39491748809814453, -0.28444138169288635, -0.18477343022823334, -0.09105003625154495, 0.0, 0.07958029955625534, 0.16093020141124725, 0.24611230194568634, 0.33791524171066284, 0.44070982933044434, 0.5626170039176941, 0.7229568362236023, 1.0)
adapter_scale = 0.5
epsilon = 1e-05

def dequantize(codes, scale_codes, second_scales):
    table = jnp.asarray(NF4_TABLE, dtype=jnp.float32)
    value_rows = jnp.take(table, codes, axis=0)
    outer = jnp.repeat(second_scales, SROWS)
    block = outer[:, None] * (scale_codes.astype(jnp.float32) + 1.0) / 256.0
    block = jnp.repeat(block, BLOCK, axis=1)
    return (value_rows * block).astype(jnp.bfloat16)

def spread_heads(value_rows, width):
    count = value_rows.shape[0]
    heads = value_rows.reshape(count, KV_HEADS, 1, HEAD)
    wide = jnp.broadcast_to(heads, (count, KV_HEADS, GROUP, HEAD)).reshape(count, KV_HEADS * GROUP * HEAD)
    filler = jnp.zeros((count, width - KV_HEADS * GROUP * HEAD), value_rows.dtype)
    return jnp.concatenate([wide, filler], axis=1)

def collapse_heads(grads):
    count = grads.shape[0]
    part = grads[:, :KV_HEADS * GROUP * HEAD].reshape(count, KV_HEADS, GROUP, HEAD)
    return lax.optimization_barrier(jnp.sum(part, axis=2)).reshape(count, KV_HEADS * HEAD)

def reference(codes, scale_codes, second_scales, gains, down_adapter, up_projection_weight, hidden_in, cotangent):
    hidden = hidden_in
    kept = []
    for layer_slot in range(LAYERS):
        frozen_base = dequantize(codes[layer_slot], scale_codes[layer_slot], second_scales[layer_slot])
        current = hidden.astype(jnp.float32)
        root_mean = jnp.sqrt(lax.optimization_barrier(jnp.mean(current * current, axis=1, keepdims=True)) + epsilon)
        gain = gains[layer_slot].astype(jnp.float32)
        normalized_input = (current / root_mean * gain).astype(jnp.bfloat16)
        narrow_product = jnp.dot(normalized_input, down_adapter[layer_slot], preferred_element_type=jnp.float32).astype(jnp.bfloat16)
        value_rows = jnp.dot(normalized_input, frozen_base, preferred_element_type=jnp.float32) + adapter_scale * jnp.dot(narrow_product, up_projection_weight[layer_slot].T, preferred_element_type=jnp.float32)
        kept.append((hidden, normalized_input, narrow_product))
        hidden = (current + spread_heads(value_rows, D)).astype(jnp.bfloat16)
    gradient = cotangent
    input_grads = []
    down_grads = []
    up_weight_gradients = []
    for layer_slot in reversed(range(LAYERS)):
        previous, normalized_input, narrow_product = kept[layer_slot]
        frozen_base = dequantize(codes[layer_slot], scale_codes[layer_slot], second_scales[layer_slot])
        current = previous.astype(jnp.float32)
        root_mean = jnp.sqrt(lax.optimization_barrier(jnp.mean(current * current, axis=1, keepdims=True)) + epsilon)
        gain = gains[layer_slot].astype(jnp.float32)
        unit = current / root_mean
        descent_vector = collapse_heads(gradient.astype(jnp.float32)).astype(jnp.bfloat16)
        up_weight_gradients.append(adapter_scale * jnp.dot(descent_vector.T, narrow_product, preferred_element_type=jnp.float32))
        narrow_gradient = (adapter_scale * jnp.dot(descent_vector, up_projection_weight[layer_slot], preferred_element_type=jnp.float32)).astype(jnp.bfloat16)
        down_grads.append(jnp.dot(normalized_input.T, narrow_gradient, preferred_element_type=jnp.float32))
        normed_grad = jnp.dot(descent_vector, frozen_base.T, preferred_element_type=jnp.float32) + jnp.dot(narrow_gradient, down_adapter[layer_slot].T, preferred_element_type=jnp.float32)
        scaled = normed_grad * gain
        hidden_grad = (scaled - unit * lax.optimization_barrier(jnp.mean(scaled * unit, axis=1, keepdims=True))) / root_mean
        gradient = (gradient.astype(jnp.float32) + hidden_grad).astype(jnp.bfloat16)
        input_grads.append(gradient)
    return (jnp.stack(input_grads[::-1]), jnp.stack(down_grads[::-1]), jnp.stack(up_weight_gradients[::-1]))
```

```python
import jax
import jax.numpy as jnp
from jax import lax
from jax.experimental import pallas as pl
from jax.experimental.pallas import tpu as pltpu
from jax.sharding import PartitionSpec as P

HEAD = 128
GROUP = 8
KV_HEADS = 4
BLOCK = 64
SROWS = 32
SPREAD = KV_HEADS * GROUP * HEAD

NF4_TABLE = (
    -1.0,
    -0.6961928009986877,
    -0.5250730514526367,
    -0.39491748809814453,
    -0.28444138169288635,
    -0.18477343022823334,
    -0.09105003625154495,
    0.0,
    0.07958029955625534,
    0.16093020141124725,
    0.24611230194568634,
    0.33791524171066284,
    0.44070982933044434,
    0.5626170039176941,
    0.7229568362236023,
    1.0,
)
adapter_scale = 0.5
epsilon = 1e-05
f32 = jnp.float32
bf16 = jnp.bfloat16


def swap(block, axis, distance):
    size = lax.axis_size(axis)
    return lax.ppermute(block, axis, [(i, i ^ distance) for i in range(size)])


def cube_gather(piece, axis, distances):
    held = [0]
    stack = piece[None]
    for distance in distances:
        arrived = swap(stack, axis, distance)
        held = held + [d ^ distance for d in held]
        stack = jnp.concatenate([stack, arrived], axis=0)
    return held, stack


def effective_rows(codes, scale_codes, second_scales, gain, down, up):
    table = jnp.zeros(codes.shape, f32)
    for entry in range(16):
        table = jnp.where(codes == entry, f32(NF4_TABLE[entry]), table)
    outer = jnp.repeat(second_scales, SROWS)
    block = outer[:, None] * (scale_codes.astype(f32) + 1.0) / 256.0
    base = (table.reshape(codes.shape[0], -1, BLOCK) * block[:, :, None]).reshape(codes.shape)
    low = adapter_scale * jnp.dot(down, up.T, preferred_element_type=f32)
    return (gain[:, None] * (base + low)).astype(bf16)


def collapse(rows):
    part = rows[:, :SPREAD].reshape(rows.shape[0], KV_HEADS, GROUP, HEAD)
    return jnp.sum(part, axis=2).reshape(rows.shape[0], KV_HEADS * HEAD)


def split_three(x):
    high = lax.reduce_precision(x, 8, 7)
    middle = lax.reduce_precision(x - high, 8, 7)
    low = x - high - middle
    return high.astype(bf16), middle.astype(bf16), low.astype(bf16)


def product(a, b):
    return jnp.dot(a, b, preferred_element_type=f32)


def product_bt(a, b):
    return lax.dot_general(a, b, (((1,), (1,)), ((), ())), preferred_element_type=f32)


def product_at(a, b):
    return lax.dot_general(a, b, (((0,), (0,)), ((), ())), preferred_element_type=f32)


def partial_products(hx, stacks, helds):
    tokens, rows = hx.shape
    parts = len(stacks)
    sections = len(helds[0])
    width = stacks[0].shape[2]
    each = rows // parts

    def kernel(hx_ref, *refs):
        out_ref = refs[-1]
        for d in range(sections):
            total = None
            for p in range(parts):
                term = product(
                    hx_ref[:, p * each : (p + 1) * each], refs[p][helds[p].index(d)]
                )
                total = term if total is None else total + term
            out_ref[d] = total.astype(bf16)

    return pl.pallas_call(
        kernel,
        out_shape=jax.ShapeDtypeStruct((sections, tokens, width), bf16),
        name="partials",
    )(hx, *stacks)


def chain(index, summed, collapsed, last, square, mixing, small, weight, hx, width):
    blocks, sections, quarter, wide = summed.shape
    value_width = mixing.shape[2]
    rank = small.shape[2] // 2
    tokens, rows = hx.shape
    groups = rows // HEAD

    def kernel(
        index_ref, sum_ref, ch_ref, last_ref, sq_ref, mix_ref, small_ref, w_ref, hx_ref,
        out_ref, gd_ref, gu_ref, v_ref, low_ref,
    ):
        me = index_ref[0]
        mine = index_ref[1]
        head = index_ref[2]
        ch = ch_ref[...]
        sq = sq_ref[...]
        total = jnp.zeros((tokens, value_width), f32)
        before = []
        inverse = []
        for m in range(sections):
            d = me ^ m
            rm2 = (
                sq
                + 2.0 * jnp.sum(total * ch, axis=1, keepdims=True)
                + GROUP * jnp.sum(total * total, axis=1, keepdims=True)
            ) / width + epsilon
            r = lax.rsqrt(rm2)
            both = sum_ref[:, d].reshape(tokens, wide).astype(f32)
            rounded = total.astype(bf16)
            v = (both[:, :value_width] + product(rounded, mix_ref[d])) * r
            low = (
                both[:, value_width : value_width + rank]
                + product(rounded, small_ref[d, :, :rank])
            ) * r
            v_ref[m] = v
            low_ref[m] = low.astype(bf16)
            before.append(rounded)
            inverse.append(r)
            total = total + v
        direction = last_ref[...].astype(f32)
        grown = jnp.zeros((tokens, rows), f32)
        for m in reversed(range(sections)):
            d = me ^ m
            r = inverse[m]
            rounded = direction.astype(bf16)
            mean = jnp.sum(rounded.astype(f32) * v_ref[m], axis=1, keepdims=True) / width
            q = mean * r * r
            scaled = (direction * r).astype(bf16)
            low_grad = (adapter_scale * product(rounded, small_ref[d, :, rank:]) * r).astype(bf16)
            gu_ref[d] = adapter_scale * product_at(low_ref[m], rounded)
            earlier = before[m].astype(f32)
            own = jnp.zeros((tokens, HEAD), f32)
            for k in range(KV_HEADS):
                own = own + jnp.where(head == k, earlier[:, k * HEAD : (k + 1) * HEAD], 0.0)
            hidden = hx_ref[...].astype(f32) + jnp.concatenate([own] * groups, axis=1)
            gd_ref[d] = product_at(low_grad, hidden.astype(bf16))
            grown = grown + product_bt(scaled, w_ref[d]) - hidden * q
            out = grown.astype(bf16).reshape(blocks, quarter, rows)
            for b in range(blocks):
                half = blocks // 2
                out_ref[m, mine ^ (2 * (b % half) + b // half)] = out[b]
            direction = direction + product_bt(scaled, mix_ref[d]) - (ch + GROUP * earlier) * q

    vmem = pl.BlockSpec(memory_space=pltpu.VMEM)
    return pl.pallas_call(
        kernel,
        in_specs=[pl.BlockSpec(memory_space=pltpu.SMEM)] + [vmem] * 8,
        out_shape=(
            jax.ShapeDtypeStruct((sections, blocks, quarter, rows), bf16),
            jax.ShapeDtypeStruct((sections, rank, rows), f32),
            jax.ShapeDtypeStruct((sections, rank, value_width), f32),
        ),
        scratch_shapes=[
            pltpu.VMEM((sections, tokens, value_width), f32),
            pltpu.VMEM((sections, tokens, rank), bf16),
        ],
        name="chain",
    )(index, summed, collapsed, last, square, mixing, small, weight, hx)


def shards(
    codes,
    scale_codes,
    second_scales,
    gains,
    down_adapter,
    up_projection_weight,
    hidden_in,
    cotangent,
):
    s = lax.axis_index("section")
    j = lax.axis_index("fsdp")
    sections = lax.axis_size("section")
    devices = lax.axis_size("fsdp")
    chips = devices // 2
    core = j % 2
    z = j // 2
    count, width = hidden_in.shape
    quarter = count // sections
    rows, value_width = codes.shape[1], codes.shape[2]
    rank = down_adapter.shape[2]
    tokens = quarter * devices
    dims = [1 << b for b in range(sections.bit_length() - 1)]

    gain = gains[0].astype(f32)
    down = down_adapter[0]
    up = up_projection_weight[0]
    gain_here = lax.dynamic_slice_in_dim(gain, j * rows, rows)
    down_here = lax.dynamic_slice_in_dim(down, j * rows, rows)
    shard = effective_rows(codes[0], scale_codes[0], second_scales[0], gain_here, down_here, up)

    half = rows // 2
    held_a, stack_a = cube_gather(shard[:half], "section", dims)
    held_b, stack_b = cube_gather(shard[half:], "section", dims[::-1])

    hq = lax.dynamic_slice_in_dim(hidden_in, s * quarter, quarter, 0)
    cq = lax.dynamic_slice_in_dim(cotangent, s * quarter, quarter, 0)
    hf = hq.astype(f32)
    ch = collapse(hf)
    ch_high = lax.reduce_precision(ch, 8, 7)
    square = jnp.sum(hf * hf, axis=1, keepdims=True)
    extra = jnp.concatenate(
        [
            ch_high.astype(bf16),
            (ch - ch_high).astype(bf16),
            collapse(cq.astype(f32)).astype(bf16),
            *split_three(square),
            jnp.zeros((quarter, HEAD - 3), bf16),
        ],
        axis=1,
    )
    arrived = []
    for d in range(chips):
        there = z ^ d
        part = lax.dynamic_slice_in_dim(hq, there * 2 * rows, 2 * rows, 1)
        part = jnp.concatenate([part, extra], axis=1)
        arrived.append(part if d == 0 else swap(part, "fsdp", 2 * d))
    arrived = jnp.stack(arrived)
    first, second = arrived[:, :, :rows], arrived[:, :, rows : 2 * rows]
    tail = arrived[:, :, 2 * rows :]
    keep = jnp.concatenate([jnp.where(core == 0, first, second), tail], axis=2)
    give = jnp.concatenate([jnp.where(core == 0, second, first), tail], axis=2)
    known = jnp.stack([keep, swap(give, "fsdp", 1)]).reshape(tokens, -1)
    hx = known[:, :rows]
    known = known[:, rows:]
    all_collapsed = known[:, :value_width].astype(f32) + known[
        :, value_width : 2 * value_width
    ].astype(f32)
    last = known[:, 2 * value_width : 3 * value_width]
    all_square = jnp.sum(
        known[:, 3 * value_width : 3 * value_width + 3].astype(f32), axis=1, keepdims=True
    )

    gained = (gain[:, None] * down.astype(f32)).astype(bf16)
    low_start = product(hidden_in, gained).astype(bf16)
    low_mix = (
        gained[:SPREAD].astype(f32).reshape(KV_HEADS, GROUP, HEAD, rank).sum(1).reshape(-1, rank)
    )
    pair = jnp.concatenate([low_mix.astype(bf16), up], axis=1)
    small = []
    starts = []
    for d in range(sections):
        part = lax.dynamic_slice_in_dim(low_start, (s ^ d) * quarter, quarter, 0)
        part = jnp.pad(part, ((0, 0), (0, 2 * rank - rank)))
        part = jnp.concatenate([pair, part], axis=0)
        part = part if d == 0 else swap(part, "section", d)
        small.append(part[:value_width])
        starts.append(part[value_width:])
    small = jnp.stack(small)
    starts = jnp.stack(starts)

    block = jnp.sum(shard.astype(f32).reshape(rows // HEAD, HEAD, value_width), axis=0)
    source = SPREAD // rows
    block = jnp.where(j < source, block, 0.0).astype(bf16)
    mixing = jnp.zeros((KV_HEADS, HEAD, value_width), bf16)
    for d in range(chips):
        got = block
        if d:
            route = [(i, i ^ (2 * d)) for i in range(source)]
            got = lax.ppermute(block, "fsdp", route)
        head = (j ^ (2 * d)) * rows // (GROUP * HEAD)
        spot = jnp.arange(KV_HEADS)[:, None, None] == head
        mixing = mixing + jnp.where(spot, got[None], jnp.zeros((), bf16))
    mixing = mixing + swap(mixing, "fsdp", 1)
    heads = KV_HEADS // 2
    mixing = lax.dynamic_slice_in_dim(mixing, core * heads, heads, 0)
    held_c, mixing = cube_gather(mixing, "section", dims)
    mixing = jnp.stack([mixing[held_c.index(d)] for d in range(sections)])
    other = swap(mixing, "fsdp", 1)
    mixing = jnp.concatenate(
        [jnp.where(core == 0, mixing, other), jnp.where(core == 0, other, mixing)], axis=1
    ).reshape(sections, value_width, value_width)

    partial = partial_products(hx, (stack_a, stack_b), (held_a, held_b))
    partial = partial.reshape(sections, 2, chips, quarter, value_width)
    over = swap(partial[:, 1], "fsdp", 1)
    on_core = (partial[:, 0].astype(f32) + over.astype(f32)).astype(bf16)
    total = on_core[:, 0].astype(f32)
    for d in range(1, chips):
        total = total + swap(on_core[:, d], "fsdp", 2 * d).astype(f32)
    total = jnp.concatenate([total.astype(bf16), starts], axis=2)
    summed = jnp.stack([total] + [swap(total, "fsdp", 2 * d) for d in range(1, chips)])
    summed = jnp.concatenate([summed, swap(summed, "fsdp", 1)], axis=0)

    weight = jnp.stack(
        [
            jnp.concatenate([stack_a[held_a.index(d)], stack_b[held_b.index(d)]], axis=0)
            for d in range(sections)
        ]
    )
    index = jnp.stack([s, j, j * rows // (GROUP * HEAD)]).astype(jnp.int32)
    grown, down_part, up_part = chain(
        index, summed, all_collapsed, last, all_square, mixing, small, weight, hx, width
    )

    per = value_width // devices
    up_part = lax.dynamic_slice_in_dim(up_part, j * per, per, 2)
    parts = jnp.concatenate([down_part, up_part], axis=2).astype(bf16)
    gradient = parts[0].astype(f32)
    for d in range(1, sections):
        gradient = gradient + swap(parts[d], "section", d).astype(f32)
    down_grad = (gradient[:, :rows] * gain_here[None, :]).T
    up_grad = gradient[:, rows:].T

    moved = grown.reshape(sections * devices, quarter, rows)
    moved = lax.all_to_all(moved, ("section", "fsdp"), 0, 0, tiled=True)
    moved = moved.reshape(sections, devices, quarter, rows).transpose(0, 2, 1, 3)
    moved = moved.reshape(count, width)
    input_grad = (cotangent.astype(f32) + moved.astype(f32)).astype(bf16)
    return (input_grad[None], down_grad[None], up_grad[None])


def solution(mesh):
    return jax.shard_map(
        shards,
        mesh=mesh,
        in_specs=(
            P("section", "fsdp", None),
            P("section", "fsdp", None),
            P("section", "fsdp"),
            P("section", None),
            P("section", None, None),
            P("section", None, None),
            P("fsdp", None),
            P("fsdp", None),
        ),
        out_specs=(
            P("section", "fsdp", None),
            P("section", "fsdp", None),
            P("section", "fsdp", None),
        ),
        check_vma=False,
    )
```

```python
import jax
import jax.numpy as jnp
from jax import lax
from jax.experimental import pallas as pl
from jax.experimental.pallas import tpu as pltpu
from jax.sharding import PartitionSpec as P

HEAD = 128
GROUP = 8
KV_HEADS = 4
BLOCK = 64
SROWS = 32
SPREAD = KV_HEADS * GROUP * HEAD

NF4_TABLE = (
    -1.0,
    -0.6961928009986877,
    -0.5250730514526367,
    -0.39491748809814453,
    -0.28444138169288635,
    -0.18477343022823334,
    -0.09105003625154495,
    0.0,
    0.07958029955625534,
    0.16093020141124725,
    0.24611230194568634,
    0.33791524171066284,
    0.44070982933044434,
    0.5626170039176941,
    0.7229568362236023,
    1.0,
)
adapter_scale = 0.5
epsilon = 1e-05
f32 = jnp.float32
bf16 = jnp.bfloat16


def swap(block, axis, distance):
    size = lax.axis_size(axis)
    return lax.ppermute(block, axis, [(i, i ^ distance) for i in range(size)])


def forwarded(halves, axis):
    first, second = {0: halves[0]}, {0: halves[1]}
    for d in range(1, lax.axis_size(axis)):
        high, low = 1 << (d.bit_length() - 1), d & -d
        if d == high:
            first[d] = swap(first[0], axis, d)
            second[d] = swap(second[0], axis, d)
    for d in range(1, lax.axis_size(axis)):
        high, low = 1 << (d.bit_length() - 1), d & -d
        if d != high:
            first[d] = swap(first[d ^ high], axis, high)
            second[d] = swap(second[d ^ low], axis, low)
    return [(first[d], second[d]) for d in range(lax.axis_size(axis))]


def product(a, b):
    return jnp.dot(a, b, preferred_element_type=f32)


def product_bt(a, b):
    return lax.dot_general(a, b, (((1,), (1,)), ((), ())), preferred_element_type=f32)


def product_at(a, b):
    return lax.dot_general(a, b, (((0,), (0,)), ((), ())), preferred_element_type=f32)


def column(row):
    parts = []
    for at in range(0, row.shape[1], HEAD):
        rows = lax.broadcasted_iota(jnp.int32, (HEAD, HEAD), 0)
        lanes = lax.broadcasted_iota(jnp.int32, (HEAD, HEAD), 1)
        spread = jnp.broadcast_to(row[:, at : at + HEAD], (HEAD, HEAD))
        parts.append(jnp.sum(jnp.where(rows == lanes, spread, 0.0), axis=1, keepdims=True))
    return jnp.concatenate(parts, axis=0)


def looked_up(codes):
    values = [f32(v) for v in NF4_TABLE]
    bit = 1
    while len(values) > 1:
        odd = (codes & bit) != 0
        values = [jnp.where(odd, values[i + 1], values[i]) for i in range(0, len(values), 2)]
        bit *= 2
    return values[0]


def effective_rows(index, codes, scale_codes, second_scales, gains, down, up):
    rows, width = codes.shape[1:]
    rank = down.shape[2]
    step = min(256, rows // 2)
    steps = rows // step
    scales = width // BLOCK

    def kernel(index_ref, code_ref, scale_ref, second_ref, gain_ref, down_ref, up_ref,
               first_ref, second_out_ref, mix_ref, acc_ref):
        i = pl.program_id(0)
        scale = scale_ref[0].astype(f32) + 1.0
        scale = second_ref[...] * scale.reshape(step // SROWS, SROWS, scales) / 256.0
        scale = scale.reshape(step, scales)
        gain = column(gain_ref[...].astype(f32))
        low = adapter_scale * product_bt(down_ref[0], up_ref[0])
        left = lax.broadcasted_iota(jnp.int32, (step, HEAD), 1) < BLOCK
        parts = []
        for g in range(width // HEAD):
            at = slice(g * HEAD, (g + 1) * HEAD)
            wide = jnp.where(left, scale[:, 2 * g : 2 * g + 1], scale[:, 2 * g + 1 : 2 * g + 2])
            parts.append((gain * (looked_up(code_ref[0, :, at]) * wide + low[:, at])).astype(bf16))
        made = jnp.concatenate(parts, axis=1)

        @pl.when(i < steps // 2)
        def _():
            first_ref[...] = made

        @pl.when(i >= steps // 2)
        def _():
            second_out_ref[...] = made

        mixed = jnp.sum(made.astype(f32).reshape(step // HEAD, HEAD, width), axis=0)

        @pl.when(i == 0)
        def _():
            acc_ref[...] = mixed

        @pl.when(i > 0)
        def _():
            acc_ref[...] += mixed

        mix_ref[...] = acc_ref[...].astype(bf16)

    half = steps // 2
    return pl.pallas_call(
        kernel,
        grid_spec=pltpu.PrefetchScalarGridSpec(
            num_scalar_prefetch=1,
            grid=(steps,),
            in_specs=[
                pl.BlockSpec((1, step, width), lambda i, ix: (0, i, 0)),
                pl.BlockSpec((1, step, scales), lambda i, ix: (0, i, 0)),
                pl.BlockSpec((step // SROWS, 1, 1), lambda i, ix: (i, 0, 0)),
                pl.BlockSpec((1, step), lambda i, ix: (0, ix[1] * steps + i)),
                pl.BlockSpec((1, step, rank), lambda i, ix: (0, ix[1] * steps + i, 0)),
                pl.BlockSpec((1, width, rank), lambda i, ix: (0, 0, 0)),
            ],
            out_specs=[
                pl.BlockSpec((step, width), lambda i, ix: (jnp.minimum(i, half - 1), 0)),
                pl.BlockSpec((step, width), lambda i, ix: (jnp.maximum(i - half, 0), 0)),
                pl.BlockSpec((HEAD, width), lambda i, ix: (0, 0)),
            ],
            scratch_shapes=[pltpu.VMEM((HEAD, width), f32)],
        ),
        out_shape=(
            jax.ShapeDtypeStruct((rows // 2, width), bf16),
            jax.ShapeDtypeStruct((rows // 2, width), bf16),
            jax.ShapeDtypeStruct((HEAD, width), bf16),
        ),
        name="effective_rows",
    )(index, codes, scale_codes, second_scales.reshape(-1, 1, 1), gains, down, up)


def hidden_parts(index, hidden, cotangent, quarter, rows, chips):
    width = hidden.shape[1]
    value_width = KV_HEADS * HEAD
    total = 2 * rows + 3 * value_width + HEAD

    def kernel(index_ref, h_ref, c_ref, *outs):
        z = index_ref[1] // 2
        core = index_ref[1] % 2
        hidden_rows = h_ref[...].astype(f32)
        square = jnp.sum(hidden_rows * hidden_rows, axis=1, keepdims=True)
        high = square.astype(bf16).astype(f32)
        middle = (square - high).astype(bf16).astype(f32)
        lane = lax.broadcasted_iota(jnp.int32, (quarter, HEAD), 1)
        squares = jnp.where(lane == 0, high, jnp.where(lane == 1, middle, square - high - middle))
        squares = jnp.where(lane < 3, squares, 0.0).astype(bf16)
        tails = [[], [], []]
        for k in range(KV_HEADS):
            ch = jnp.zeros((quarter, HEAD), f32)
            cc = jnp.zeros((quarter, HEAD), f32)
            for g in range(GROUP):
                at = slice((k * GROUP + g) * HEAD, (k * GROUP + g + 1) * HEAD)
                ch = ch + hidden_rows[:, at]
                cc = cc + c_ref[:, at].astype(f32)
            near = ch.astype(bf16)
            tails[0].append(near)
            tails[1].append((ch - near.astype(f32)).astype(bf16))
            tails[2].append(cc.astype(bf16))
        tail = jnp.concatenate(tails[0] + tails[1] + tails[2] + [squares], axis=1)
        for d in range(chips):
            there = 2 * (z ^ d)
            keep = pl.multiple_of((there + core) * rows, HEAD)
            give = pl.multiple_of((there + 1 - core) * rows, HEAD)
            outs[d][:, :rows] = h_ref[:, pl.ds(keep, rows)]
            outs[d][:, rows : 2 * rows] = h_ref[:, pl.ds(give, rows)]
            outs[d][:, 2 * rows :] = tail

    return pl.pallas_call(
        kernel,
        grid_spec=pltpu.PrefetchScalarGridSpec(
            num_scalar_prefetch=1,
            grid=(1,),
            in_specs=[
                pl.BlockSpec((quarter, width), lambda i, ix: (ix[0], 0)),
                pl.BlockSpec((quarter, SPREAD), lambda i, ix: (ix[0], 0)),
            ],
            out_specs=[pl.BlockSpec((quarter, total), lambda i, ix: (0, 0))] * chips,
        ),
        out_shape=[jax.ShapeDtypeStruct((quarter, total), bf16)] * chips,
        name="hidden_parts",
    )(index, hidden, cotangent)


def given_parts(parts, rows):
    quarter, total = parts[0].shape

    def kernel(*refs):
        for d, ref in enumerate(refs[:-1]):
            refs[-1][d] = ref[:, rows:]

    return pl.pallas_call(
        kernel,
        out_shape=jax.ShapeDtypeStruct((len(parts), quarter, total - rows), bf16),
        name="given_parts",
    )(*parts)


def low_rank_parts(index, hidden, gains, down, up, quarter, sections):
    count, width = hidden.shape
    rank = down.shape[2]
    value_width = up.shape[1]
    chunk = GROUP * HEAD

    def kernel(index_ref, h_ref, gain_ref, down_ref, up_ref, *refs):
        outs, low_ref = refs[:-1], refs[-1]
        low = jnp.zeros((count, rank), f32)
        mixes = []
        for k in range(width // chunk):
            at = slice(k * chunk, (k + 1) * chunk)
            gain = column(gain_ref[:, at].astype(f32))
            gained = (gain * down_ref[0, at, :].astype(f32)).astype(bf16)
            low = low + product(h_ref[:, at], gained)
            if k < KV_HEADS:
                mixes.append(jnp.sum(gained.astype(f32).reshape(GROUP, HEAD, rank), axis=0))
        low_ref[...] = jnp.concatenate([low, jnp.zeros((count, HEAD - rank), f32)], axis=1)
        pair = jnp.concatenate([jnp.concatenate(mixes, axis=0).astype(bf16), up_ref[0]], axis=1)
        for d in range(sections):
            outs[d][:value_width] = pair
            start = pl.multiple_of((index_ref[0] ^ d) * quarter, quarter)
            outs[d][value_width:] = low_ref[pl.ds(start, quarter)].astype(bf16)

    vmem = pl.BlockSpec(memory_space=pltpu.VMEM)
    return pl.pallas_call(
        kernel,
        in_specs=[pl.BlockSpec(memory_space=pltpu.SMEM)] + [vmem] * 4,
        out_shape=[jax.ShapeDtypeStruct((value_width + quarter, HEAD), bf16)] * sections,
        scratch_shapes=[pltpu.VMEM((count, HEAD), f32)],
        name="low_rank_parts",
    )(index, hidden, gains, down, up)


def partial_products(parts, given, weights, rows):
    chips = len(parts)
    quarter = parts[0].shape[0]
    sections = len(weights)
    width = weights[0][0].shape[1]
    half = rows // 2
    tokens = chips * quarter

    def kernel(*refs):
        part_refs, given_ref = refs[:chips], refs[chips]
        weight_refs = refs[chips + 1 : -2]
        own = jnp.concatenate([ref[:, :rows] for ref in part_refs], axis=0)
        other = given_ref[:, :, :rows].reshape(tokens, rows)
        both = jnp.concatenate([own, other], axis=0)
        for d in range(sections):
            made = product(both[:, :half], weight_refs[2 * d][...])
            made = made + product(both[:, half:], weight_refs[2 * d + 1][...])
            made = made.astype(bf16).reshape(2, chips, quarter, width)
            refs[-2][:, d] = made[0]
            refs[-1][:, d] = made[1]

    shape = jax.ShapeDtypeStruct((chips, sections, quarter, width), bf16)
    flat = [piece for pair in weights for piece in pair]
    return pl.pallas_call(kernel, out_shape=(shape, shape), name="partials")(*parts, given, *flat)


def sum_cores(mine, other):
    chips = mine.shape[0]

    def kernel(a_ref, b_ref, *outs):
        for d in range(chips):
            outs[d][...] = (a_ref[d].astype(f32) + b_ref[d].astype(f32)).astype(bf16)

    return pl.pallas_call(
        kernel,
        out_shape=[jax.ShapeDtypeStruct(mine.shape[1:], bf16)] * chips,
        name="sum_cores",
    )(mine, other)


def sum_chips(pieces, smalls):
    sections, quarter, width = pieces[0].shape

    def kernel(*refs):
        total = refs[0][...].astype(f32)
        for ref in refs[1 : len(pieces)]:
            total = total + ref[...].astype(f32)
        refs[-1][:, :, :width] = total.astype(bf16)
        for d in range(sections):
            refs[-1][d, :, width:] = refs[len(pieces) + d][width:]

    return pl.pallas_call(
        kernel,
        out_shape=jax.ShapeDtypeStruct((sections, quarter, width + HEAD), bf16),
        name="sum_chips",
    )(*pieces, *smalls)


def chain(index, sums, parts, own_given, given, mixings, smalls, weights, rows, width):
    blocks = len(sums)
    chips = len(parts)
    sections, quarter, wide = sums[0].shape
    value_width = mixings[0].shape[1]
    rank = HEAD // 2
    tokens = blocks * quarter
    groups = rows // HEAD
    half = rows // 2

    def kernel(index_ref, *refs):
        refs = list(refs)
        take = lambda n: [refs.pop(0) for _ in range(n)]
        sum_refs, part_refs = take(blocks), take(chips)
        (own_ref, given_ref) = take(2)
        mix_in, small_in, weight_in = take(sections), take(sections), take(2 * sections)
        (out_ref,) = take(1)
        grad_refs = take(sections)
        v_ref, mix_ref, small_ref, w_ref, grad_ref, sems = take(6)
        me = index_ref[0]
        mine = index_ref[1]
        head = index_ref[2]
        copies = {}
        for d in range(sections):
            m = me ^ d
            copies["mix", d] = pltpu.make_async_copy(mix_in[d], mix_ref.at[m], sems.at[0, d])
            copies["small", d] = pltpu.make_async_copy(
                small_in[d].at[pl.ds(0, value_width)], small_ref.at[m], sems.at[1, d]
            )
            for p in range(2):
                copies["w", p, d] = pltpu.make_async_copy(
                    weight_in[2 * d + p], w_ref.at[m, pl.ds(p * half, half)], sems.at[2 + p, d]
                )
        for copy in copies.values():
            copy.start()
        tail = jnp.concatenate(
            [
                own_ref[:, :, rows:].reshape(tokens // 2, -1),
                given_ref[:, :, rows:].reshape(tokens // 2, -1),
            ],
            axis=0,
        )
        hx = jnp.concatenate(
            [ref[:, :rows] for ref in part_refs]
            + [given_ref[:, :, :rows].reshape(tokens // 2, rows)],
            axis=0,
        ).astype(f32)
        ch = tail[:, :value_width].astype(f32) + tail[:, value_width : 2 * value_width].astype(f32)
        sq = jnp.sum(tail[:, 3 * value_width :].astype(f32), axis=1, keepdims=True)
        for d in range(sections):
            copies["mix", d].wait()
            copies["small", d].wait()
        total = jnp.zeros((tokens, value_width), f32)
        before, inverse, lows = [], [], []
        for m in range(sections):
            d = me ^ m
            rm2 = (
                sq
                + 2.0 * jnp.sum(total * ch, axis=1, keepdims=True)
                + GROUP * jnp.sum(total * total, axis=1, keepdims=True)
            ) / width + epsilon
            r = lax.rsqrt(rm2)
            both = jnp.concatenate([ref[d] for ref in sum_refs], axis=0).astype(f32)
            rounded = total.astype(bf16)
            v = (both[:, :value_width] + product(rounded, mix_ref[m])) * r
            low = both[:, value_width : value_width + rank] + product(
                rounded, small_ref[m, :, :rank]
            )
            v_ref[m] = v
            lows.append((low * r).astype(bf16))
            before.append(rounded)
            inverse.append(r)
            total = total + v
        for d in range(sections):
            for p in range(2):
                copies["w", p, d].wait()
        direction = tail[:, 2 * value_width : 3 * value_width].astype(f32)
        grown = jnp.zeros((tokens, rows), f32)
        for m in reversed(range(sections)):
            r = inverse[m]
            rounded = direction.astype(bf16)
            mean = jnp.sum(rounded.astype(f32) * v_ref[m], axis=1, keepdims=True) / width
            q = mean * r * r
            scaled = (direction * r).astype(bf16)
            low_grad = adapter_scale * product(rounded, small_ref[m, :, rank:]) * r
            grad_ref[m, :, rows:] = (adapter_scale * product_at(lows[m], rounded)).astype(bf16)
            earlier = before[m].astype(f32)
            own = jnp.zeros((tokens, HEAD), f32)
            for k in range(KV_HEADS):
                own = own + jnp.where(head == k, earlier[:, k * HEAD : (k + 1) * HEAD], 0.0)
            hidden = hx + jnp.concatenate([own] * groups, axis=1)
            grad_ref[m, :, :rows] = product_at(
                low_grad.astype(bf16), hidden.astype(bf16)
            ).astype(bf16)
            grown = grown + product_bt(scaled, w_ref[m]) - hidden * q
            out = grown.astype(bf16).reshape(blocks, quarter, rows)
            for b in range(blocks):
                out_ref[m, mine ^ (2 * (b % chips) + b // chips)] = out[b]
            direction = direction + product_bt(scaled, mix_ref[m]) - (ch + GROUP * earlier) * q
        for d in range(sections):
            grad_refs[d][...] = grad_ref[me ^ d]

    vmem = pl.BlockSpec(memory_space=pltpu.VMEM)
    anywhere = pl.BlockSpec(memory_space=pl.ANY)
    flat = [piece for pair in weights for piece in pair]
    grad_width = rows + value_width
    outs = pl.pallas_call(
        kernel,
        in_specs=[pl.BlockSpec(memory_space=pltpu.SMEM)]
        + [vmem] * (blocks + chips + 2)
        + [anywhere] * (4 * sections),
        out_shape=[jax.ShapeDtypeStruct((sections, blocks, quarter, rows), bf16)]
        + [jax.ShapeDtypeStruct((rank, grad_width), bf16)] * sections,
        scratch_shapes=[
            pltpu.VMEM((sections, tokens, value_width), f32),
            pltpu.VMEM((sections, value_width, value_width), bf16),
            pltpu.VMEM((sections, value_width, HEAD), bf16),
            pltpu.VMEM((sections, rows, value_width), bf16),
            pltpu.VMEM((sections, rank, grad_width), bf16),
            pltpu.SemaphoreType.DMA((4, sections)),
        ],
        name="chain",
    )(index, *sums, *parts, own_given, given, *mixings, *smalls, *flat)
    return outs[0], outs[1:]


def placed(moved, cotangent):
    sections, devices, quarter, rows = moved.shape
    count, width = cotangent.shape

    def kernel(m_ref, c_ref, out_ref):
        for j in range(devices):
            at = slice(j * rows, (j + 1) * rows)
            out_ref[0, :, at] = (c_ref[:, at].astype(f32) + m_ref[0, j].astype(f32)).astype(bf16)

    return pl.pallas_call(
        kernel,
        grid=(sections,),
        in_specs=[
            pl.BlockSpec((1, devices, quarter, rows), lambda i: (i, 0, 0, 0)),
            pl.BlockSpec((quarter, width), lambda i: (i, 0)),
        ],
        out_specs=pl.BlockSpec((1, quarter, width), lambda i: (0, i, 0)),
        out_shape=jax.ShapeDtypeStruct((1, count, width), bf16),
        name="placed",
    )(moved, cotangent)


def shards(
    codes,
    scale_codes,
    second_scales,
    gains,
    down_adapter,
    up_projection_weight,
    hidden_in,
    cotangent,
):
    s = lax.axis_index("section")
    j = lax.axis_index("fsdp")
    sections = lax.axis_size("section")
    devices = lax.axis_size("fsdp")
    chips = devices // 2
    count, width = hidden_in.shape
    quarter = count // sections
    rows, value_width = codes.shape[1], codes.shape[2]
    index = jnp.stack([s, j, j * rows // (GROUP * HEAD)]).astype(jnp.int32)

    first, second, block = effective_rows(
        index, codes, scale_codes, second_scales, gains, down_adapter, up_projection_weight
    )
    weights = forwarded((first, second), "section")

    parts = hidden_parts(index, hidden_in, cotangent, quarter, rows, chips)
    parts = [part if d == 0 else swap(part, "fsdp", 2 * d) for d, part in enumerate(parts)]
    own_given = given_parts(parts, rows)
    given = swap(own_given, "fsdp", 1)

    smalls = low_rank_parts(
        index, hidden_in, gains, down_adapter, up_projection_weight, quarter, sections
    )
    smalls = [small if d == 0 else swap(small, "section", d) for d, small in enumerate(smalls)]

    source = SPREAD // rows
    mixing = jnp.zeros((KV_HEADS, HEAD, value_width), bf16)
    for d in range(chips):
        got = block
        if d:
            got = lax.ppermute(block, "fsdp", [(i, i ^ (2 * d)) for i in range(source)])
        head = (j ^ (2 * d)) * rows // (GROUP * HEAD)
        spot = jnp.arange(KV_HEADS)[:, None, None] == head
        mixing = mixing + jnp.where(spot, got[None], jnp.zeros((), bf16))
    mixing = (mixing + swap(mixing, "fsdp", 1)).reshape(value_width, value_width)
    mixings = [mixing] + [swap(mixing, "section", d) for d in range(1, sections)]

    mine, other = partial_products(parts, given, weights, rows)
    pieces = sum_cores(mine, swap(other, "fsdp", 1))
    pieces = [piece if d == 0 else swap(piece, "fsdp", 2 * d) for d, piece in enumerate(pieces)]
    total = sum_chips(pieces, smalls)
    sums = [total if d == 0 else swap(total, "fsdp", 2 * d) for d in range(chips)]
    sums = sums + [swap(part, "fsdp", 1) for part in sums]

    grown, grads = chain(
        index, sums, parts, own_given, given, mixings, smalls, weights, rows, width
    )

    gradient = grads[0].astype(f32)
    for d in range(1, sections):
        gradient = gradient + swap(grads[d], "section", d).astype(f32)
    per = value_width // devices
    gain_here = lax.dynamic_slice_in_dim(gains[0].astype(f32), j * rows, rows)
    down_grad = (gradient[:, :rows] * gain_here[None, :]).T
    up_grad = lax.dynamic_slice_in_dim(gradient[:, rows:], j * per, per, 1).T

    moved = grown.reshape(sections * devices, quarter, rows)
    moved = lax.all_to_all(moved, ("section", "fsdp"), 0, 0, tiled=True)
    input_grad = placed(moved.reshape(sections, devices, quarter, rows), cotangent)
    return (input_grad, down_grad[None], up_grad[None])


def solution(mesh):
    return jax.shard_map(
        shards,
        mesh=mesh,
        in_specs=(
            P("section", "fsdp", None),
            P("section", "fsdp", None),
            P("section", "fsdp"),
            P("section", None),
            P("section", None, None),
            P("section", None, None),
            P("fsdp", None),
            P("fsdp", None),
        ),
        out_specs=(
            P("section", "fsdp", None),
            P("section", "fsdp", None),
            P("section", "fsdp", None),
        ),
        check_vma=False,
    )
```

```python
import jax
import jax.numpy as jnp
from jax import lax
from jax.experimental import pallas as pl
from jax.experimental.pallas import tpu as pltpu
from jax.sharding import PartitionSpec as P

HEAD = 128
GROUP = 8
KV_HEADS = 4
BLOCK = 64
SROWS = 32
SPREAD = KV_HEADS * GROUP * HEAD

NF4_TABLE = (
    -1.0,
    -0.6961928009986877,
    -0.5250730514526367,
    -0.39491748809814453,
    -0.28444138169288635,
    -0.18477343022823334,
    -0.09105003625154495,
    0.0,
    0.07958029955625534,
    0.16093020141124725,
    0.24611230194568634,
    0.33791524171066284,
    0.44070982933044434,
    0.5626170039176941,
    0.7229568362236023,
    1.0,
)
adapter_scale = 0.5
epsilon = 1e-05
f32 = jnp.float32
bf16 = jnp.bfloat16


def swap(block, axis, distance):
    size = lax.axis_size(axis)
    return lax.ppermute(block, axis, [(i, i ^ distance) for i in range(size)])


def exchange(blocks, axis):
    return lax.all_to_all(blocks, axis, 0, 0, tiled=True)


def forwarded(halves, axis):
    first, second = {0: halves[0]}, {0: halves[1]}
    for d in range(1, lax.axis_size(axis)):
        high, low = 1 << (d.bit_length() - 1), d & -d
        if d == high:
            first[d] = swap(first[0], axis, d)
            second[d] = swap(second[0], axis, d)
    for d in range(1, lax.axis_size(axis)):
        high, low = 1 << (d.bit_length() - 1), d & -d
        if d != high:
            first[d] = swap(first[d ^ high], axis, high)
            second[d] = swap(second[d ^ low], axis, low)
    return [(first[d], second[d]) for d in range(lax.axis_size(axis))]


def product(a, b):
    return jnp.dot(a, b, preferred_element_type=f32)


def product_bt(a, b):
    return lax.dot_general(a, b, (((1,), (1,)), ((), ())), preferred_element_type=f32)


def product_at(a, b):
    return lax.dot_general(a, b, (((0,), (0,)), ((), ())), preferred_element_type=f32)


def looked_up(codes):
    values = [f32(v) for v in NF4_TABLE]
    bit = 1
    while len(values) > 1:
        odd = (codes & bit) != 0
        values = [jnp.where(odd, values[i + 1], values[i]) for i in range(0, len(values), 2)]
        bit *= 2
    return values[0]


def effective_rows(index, codes, scale_codes, second_scales, gains, down, up):
    rows, width = codes.shape[1:]
    rank = down.shape[1]
    step = min(256, rows // 2)
    steps = rows // step
    scales = width // BLOCK

    def kernel(index_ref, code_ref, scale_ref, second_ref, gain_ref, down_ref, up_ref,
               first_ref, last_ref, mix_ref, acc_ref):
        i = pl.program_id(0)
        lane = lax.broadcasted_iota(jnp.int32, (1, step), 1) // SROWS
        second = jnp.zeros((1, step), f32)
        for g in range(step // SROWS):
            second = jnp.where(lane == g, second_ref[0, i * (step // SROWS) + g], second)
        gain = gain_ref[...].astype(f32)
        factor = second * (scale_ref[0].astype(f32) + 1.0) / 256.0 * gain
        near = factor.astype(bf16)
        rest = (factor - near.astype(f32)).astype(bf16)
        at_block = lax.broadcasted_iota(jnp.int32, (2 * scales, width), 1) // BLOCK
        row = lax.broadcasted_iota(jnp.int32, (2 * scales, width), 0) % scales
        expand = jnp.where(at_block == row, 1.0, 0.0).astype(bf16)
        wide = product_at(jnp.concatenate([near, rest], axis=0), expand)
        gained = (gain * adapter_scale * down_ref[0].astype(f32)).astype(bf16)
        low = product_at(gained, up_ref[0])
        made = (looked_up(code_ref[0]) * wide + low).astype(bf16)

        @pl.when(i < steps // 2)
        def _():
            first_ref[...] = made

        @pl.when(i >= steps // 2)
        def _():
            last_ref[...] = made

        mixed = jnp.sum(made.astype(f32).reshape(step // HEAD, HEAD, width), axis=0)

        @pl.when(i == 0)
        def _():
            acc_ref[...] = mixed

        @pl.when(i > 0)
        def _():
            acc_ref[...] += mixed

        @pl.when(i == steps - 1)
        def _():
            for copy in range(mix_ref.shape[0]):
                mix_ref[copy] = acc_ref[...].astype(bf16)

    half = steps // 2
    devices = gains.shape[1] // rows
    return pl.pallas_call(
        kernel,
        grid_spec=pltpu.PrefetchScalarGridSpec(
            num_scalar_prefetch=1,
            grid=(steps,),
            in_specs=[
                pl.BlockSpec((1, step, width), lambda i, ix: (0, i, 0)),
                pl.BlockSpec((1, scales, step), lambda i, ix: (0, 0, i)),
                pl.BlockSpec(memory_space=pltpu.SMEM),
                pl.BlockSpec((1, step), lambda i, ix: (0, ix[1] * steps + i)),
                pl.BlockSpec((1, rank, step), lambda i, ix: (0, 0, ix[1] * steps + i)),
                pl.BlockSpec((1, rank, width), lambda i, ix: (0, 0, 0)),
            ],
            out_specs=[
                pl.BlockSpec((step, width), lambda i, ix: (jnp.minimum(i, half - 1), 0)),
                pl.BlockSpec((step, width), lambda i, ix: (jnp.maximum(i - half, 0), 0)),
                pl.BlockSpec((devices, HEAD, width), lambda i, ix: (0, 0, 0)),
            ],
            scratch_shapes=[pltpu.VMEM((HEAD, width), f32)],
        ),
        out_shape=(
            jax.ShapeDtypeStruct((rows // 2, width), bf16),
            jax.ShapeDtypeStruct((rows // 2, width), bf16),
            jax.ShapeDtypeStruct((devices, HEAD, width), bf16),
        ),
        name="effective_rows",
    )(index, codes, scale_codes, second_scales, gains, down, up)


def hidden_parts(index, hidden, cotangent, quarter, rows, chips):
    width = hidden.shape[1]
    value_width = KV_HEADS * HEAD
    total = 2 * rows + 3 * value_width + HEAD

    def kernel(index_ref, h_ref, c_ref, out_ref):
        core = index_ref[1] % 2
        hidden_rows = h_ref[...].astype(f32)
        square = jnp.sum(hidden_rows * hidden_rows, axis=1, keepdims=True)
        high = square.astype(bf16).astype(f32)
        middle = (square - high).astype(bf16).astype(f32)
        lane = lax.broadcasted_iota(jnp.int32, (quarter, HEAD), 1)
        squares = jnp.where(lane == 0, high, jnp.where(lane == 1, middle, square - high - middle))
        squares = jnp.where(lane < 3, squares, 0.0).astype(bf16)
        tails = [[], [], []]
        for k in range(KV_HEADS):
            ch = jnp.zeros((quarter, HEAD), f32)
            cc = jnp.zeros((quarter, HEAD), f32)
            for g in range(GROUP):
                at = slice((k * GROUP + g) * HEAD, (k * GROUP + g + 1) * HEAD)
                ch = ch + hidden_rows[:, at]
                cc = cc + c_ref[:, at].astype(f32)
            near = ch.astype(bf16)
            tails[0].append(near)
            tails[1].append((ch - near.astype(f32)).astype(bf16))
            tails[2].append(cc.astype(bf16))
        tail = jnp.concatenate(tails[0] + tails[1] + tails[2] + [squares], axis=1)
        for z in range(chips):
            keep = pl.multiple_of((2 * z + core) * rows, HEAD)
            give = pl.multiple_of((2 * z + 1 - core) * rows, HEAD)
            out_ref[z, :, :rows] = h_ref[:, pl.ds(keep, rows)]
            out_ref[z, :, rows : 2 * rows] = h_ref[:, pl.ds(give, rows)]
            out_ref[z, :, 2 * rows :] = tail

    return pl.pallas_call(
        kernel,
        grid_spec=pltpu.PrefetchScalarGridSpec(
            num_scalar_prefetch=1,
            grid=(1,),
            in_specs=[
                pl.BlockSpec((quarter, width), lambda i, ix: (ix[0], 0)),
                pl.BlockSpec((quarter, SPREAD), lambda i, ix: (ix[0], 0)),
            ],
            out_specs=pl.BlockSpec((chips, quarter, total), lambda i, ix: (0, 0, 0)),
        ),
        out_shape=jax.ShapeDtypeStruct((chips, quarter, total), bf16),
        name="hidden_parts",
    )(index, hidden, cotangent)


def low_rank_parts(index, hidden, gains, down, up, quarter, sections):
    count, width = hidden.shape
    rank = down.shape[1]
    value_width = up.shape[2]
    chunk = GROUP * HEAD

    def kernel(h_ref, gain_ref, down_ref, up_ref, out_ref):
        low = jnp.zeros((count, rank), f32)
        mixes = []
        for k in range(width // chunk):
            at = slice(k * chunk, (k + 1) * chunk)
            gained = (gain_ref[:, at].astype(f32) * down_ref[0, :, at].astype(f32)).astype(bf16)
            low = low + product_bt(h_ref[:, at], gained)
            if k < KV_HEADS:
                parts = [gained[:, g * HEAD : (g + 1) * HEAD].astype(f32) for g in range(GROUP)]
                mixes.append(sum(parts[1:], parts[0]))
        mixed = jnp.concatenate(mixes, axis=1).astype(bf16)
        low = jnp.concatenate([low, jnp.zeros((count, value_width - rank), f32)], axis=1)
        low = low.astype(bf16)
        for t in range(sections):
            out_ref[t, :rank] = mixed
            out_ref[t, rank : 2 * rank] = up_ref[0]
            out_ref[t, 2 * rank :] = low[t * quarter : (t + 1) * quarter]

    shape = (sections, 2 * rank + quarter, value_width)
    return pl.pallas_call(
        kernel, out_shape=jax.ShapeDtypeStruct(shape, bf16), name="low_rank_parts"
    )(hidden, gains, down, up)


def mixing_copies(blocks, sections, source):
    width = blocks.shape[2]
    each = source // KV_HEADS

    def kernel(b_ref, out_ref):
        for k in range(KV_HEADS):
            made = b_ref[k * each]
            for i in range(1, each):
                made = (made.astype(f32) + b_ref[k * each + i].astype(f32)).astype(bf16)
            for t in range(sections):
                out_ref[t, k * HEAD : (k + 1) * HEAD] = made

    return pl.pallas_call(
        kernel,
        out_shape=jax.ShapeDtypeStruct((sections, KV_HEADS * HEAD, width), bf16),
        name="mixing_copies",
    )(blocks)


def partial_products(own, given, weights, rows):
    chips, quarter = own.shape[:2]
    sections = len(weights)
    width = weights[0][0].shape[1]
    half = rows // 2
    tokens = chips * quarter

    def kernel(*refs):
        own_ref, given_ref = refs[:2]
        weight_refs = refs[2:-2]
        left = own_ref[:, :, :rows].reshape(tokens, rows)
        right = given_ref[:, :, rows : 2 * rows].reshape(tokens, rows)
        both = jnp.concatenate([left, right], axis=0)
        for d in range(sections):
            made = product(both[:, :half], weight_refs[2 * d][...])
            made = made + product(both[:, half:], weight_refs[2 * d + 1][...])
            made = made.astype(bf16).reshape(2, chips, quarter, width)
            refs[-2][:, d] = made[0]
            refs[-1][:, d] = made[1]

    shape = jax.ShapeDtypeStruct((chips, sections, quarter, width), bf16)
    flat = [piece for pair in weights for piece in pair]
    return pl.pallas_call(kernel, out_shape=(shape, shape), name="partials")(own, given, *flat)


def sum_cores(mine, other):
    def kernel(a_ref, b_ref, out_ref):
        out_ref[...] = (a_ref[...].astype(f32) + b_ref[...].astype(f32)).astype(bf16)

    return pl.pallas_call(
        kernel, out_shape=jax.ShapeDtypeStruct(mine.shape, bf16), name="sum_cores"
    )(mine, other)


def sum_chips(index, pieces, small):
    chips, sections, quarter, width = pieces.shape
    skip = small.shape[1] - quarter

    def kernel(index_ref, p_ref, small_ref, out_ref):
        total = p_ref[0].astype(f32)
        for z in range(1, chips):
            total = total + p_ref[z].astype(f32)
        total = total.astype(bf16)
        for z in range(chips):
            out_ref[z, :, :, :width] = total
            for d in range(sections):
                out_ref[z, d, :, width:] = small_ref[index_ref[0] ^ d, skip:, :HEAD]

    vmem = pl.BlockSpec(memory_space=pltpu.VMEM)
    return pl.pallas_call(
        kernel,
        in_specs=[pl.BlockSpec(memory_space=pltpu.SMEM), vmem, vmem],
        out_shape=jax.ShapeDtypeStruct((chips, sections, quarter, width + HEAD), bf16),
        name="sum_chips",
    )(index, pieces, small)


def chain(index, sums, other_sums, own, given, mixing, small, weights, rows, width):
    chips, sections, quarter, wide = sums.shape
    value_width = mixing.shape[1]
    rank = HEAD // 2
    tokens = 2 * chips * quarter
    groups = rows // HEAD
    half = rows // 2

    def kernel(index_ref, *refs):
        refs = list(refs)
        take = lambda n: [refs.pop(0) for _ in range(n)]
        sum_ref, other_ref, own_ref, given_ref, small_ref, mix_in = take(6)
        weight_in = take(2 * sections)
        out_ref, grad_ref = take(2)
        v_ref, mix_ref, w_ref, mix_sem, sems = take(5)
        me = index_ref[0]
        core = index_ref[1] % 2
        head = index_ref[2]
        mix_copy = pltpu.make_async_copy(mix_in, mix_ref, mix_sem)
        mix_copy.start()
        copies = []
        for d in range(sections):
            for p in range(2):
                copies.append(
                    pltpu.make_async_copy(
                        weight_in[2 * d + p],
                        w_ref.at[me ^ d, pl.ds(p * half, half)],
                        sems.at[p, d],
                    )
                )
        for copy in copies:
            copy.start()

        def both(left, right):
            merged = jnp.concatenate([left, right], axis=0)
            return merged.reshape(tokens, merged.shape[-1])

        tail = both(own_ref[:, :, 2 * rows :], given_ref[:, :, 2 * rows :])
        hx = both(own_ref[:, :, :rows], given_ref[:, :, rows : 2 * rows]).astype(f32)
        ch = tail[:, :value_width].astype(f32) + tail[:, value_width : 2 * value_width].astype(f32)
        sq = jnp.sum(tail[:, 3 * value_width :].astype(f32), axis=1, keepdims=True)
        mix_copy.wait()
        total = jnp.zeros((tokens, value_width), f32)
        before, inverse, lows = [], [], []
        for m in range(sections):
            d = me ^ m
            rm2 = (
                sq
                + 2.0 * jnp.sum(total * ch, axis=1, keepdims=True)
                + GROUP * jnp.sum(total * total, axis=1, keepdims=True)
            ) / width + epsilon
            r = lax.rsqrt(rm2)
            start = both(sum_ref[:, d], other_ref[:, d]).astype(f32)
            rounded = total.astype(bf16)
            v = (start[:, :value_width] + product(rounded, mix_ref[m])) * r
            low = start[:, value_width : value_width + rank]
            low = low + product_bt(rounded, small_ref[m, :rank])
            v_ref[m] = v
            lows.append((low * r).astype(bf16))
            before.append(rounded)
            inverse.append(r)
            total = total + v
        for copy in copies:
            copy.wait()
        direction = tail[:, 2 * value_width : 3 * value_width].astype(f32)
        grown = jnp.zeros((tokens, rows), f32)
        for m in reversed(range(sections)):
            r = inverse[m]
            rounded = direction.astype(bf16)
            mean = jnp.sum(rounded.astype(f32) * v_ref[m], axis=1, keepdims=True) / width
            q = mean * r * r
            scaled = (direction * r).astype(bf16)
            low_grad = adapter_scale * product_bt(rounded, small_ref[m, rank : 2 * rank]) * r
            grad_ref[m, :, rows:] = (adapter_scale * product_at(lows[m], rounded)).astype(bf16)
            earlier = before[m].astype(f32)
            spread = jnp.zeros((tokens, HEAD), f32)
            for k in range(KV_HEADS):
                spread = spread + jnp.where(head == k, earlier[:, k * HEAD : (k + 1) * HEAD], 0.0)
            hidden = hx + jnp.concatenate([spread] * groups, axis=1)
            grad_ref[m, :, :rows] = product_at(
                low_grad.astype(bf16), hidden.astype(bf16)
            ).astype(bf16)
            grown = grown + product_bt(scaled, w_ref[m]) - hidden * q
            out = grown.astype(bf16).reshape(2, chips, quarter, rows)
            for e in range(2):
                for z in range(chips):
                    out_ref[m, 2 * z + (core ^ e)] = out[e, z]
            direction = direction + product_bt(scaled, mix_ref[m]) - (ch + GROUP * earlier) * q

    vmem = pl.BlockSpec(memory_space=pltpu.VMEM)
    anywhere = pl.BlockSpec(memory_space=pl.ANY)
    flat = [piece for pair in weights for piece in pair]
    grad_width = rows + value_width
    return pl.pallas_call(
        kernel,
        in_specs=[pl.BlockSpec(memory_space=pltpu.SMEM)]
        + [vmem] * 5
        + [anywhere] * (1 + 2 * sections),
        out_shape=(
            jax.ShapeDtypeStruct((sections, 2 * chips, quarter, rows), bf16),
            jax.ShapeDtypeStruct((sections, rank, grad_width), bf16),
        ),
        scratch_shapes=[
            pltpu.VMEM((sections, tokens, value_width), f32),
            pltpu.VMEM((sections, value_width, value_width), bf16),
            pltpu.VMEM((sections, rows, value_width), bf16),
            pltpu.SemaphoreType.DMA,
            pltpu.SemaphoreType.DMA((2, sections)),
        ],
        name="chain",
    )(index, sums, other_sums, own, given, small, mixing, *flat)


def placed(moved, cotangent):
    sections, devices, quarter, rows = moved.shape
    count, width = cotangent.shape

    def kernel(m_ref, c_ref, out_ref):
        for j in range(devices):
            at = slice(j * rows, (j + 1) * rows)
            out_ref[0, :, at] = (c_ref[:, at].astype(f32) + m_ref[0, j].astype(f32)).astype(bf16)

    return pl.pallas_call(
        kernel,
        grid=(sections,),
        in_specs=[
            pl.BlockSpec((1, devices, quarter, rows), lambda i: (i, 0, 0, 0)),
            pl.BlockSpec((quarter, width), lambda i: (i, 0)),
        ],
        out_specs=pl.BlockSpec((1, quarter, width), lambda i: (0, i, 0)),
        out_shape=jax.ShapeDtypeStruct((1, count, width), bf16),
        name="placed",
    )(moved, cotangent)


def shards(
    codes,
    scale_codes,
    second_scales,
    gains,
    down_adapter,
    up_projection_weight,
    hidden_in,
    cotangent,
):
    fsdp = ("chip", "core")
    s = lax.axis_index("section")
    j = lax.axis_index(fsdp)
    sections = lax.axis_size("section")
    chips = lax.axis_size("chip")
    devices = lax.axis_size(fsdp)
    count, width = hidden_in.shape
    quarter = count // sections
    rows, value_width = codes.shape[1], codes.shape[2]
    index = jnp.stack([s, j, j * rows // (GROUP * HEAD)]).astype(jnp.int32)
    scale_codes = jnp.swapaxes(scale_codes, 1, 2)
    down = jnp.swapaxes(down_adapter, 1, 2)
    up = jnp.swapaxes(up_projection_weight, 1, 2)

    first, second, block = effective_rows(
        index, codes, scale_codes, second_scales, gains, down, up
    )
    weights = forwarded((first, second), "section")

    own = exchange(hidden_parts(index, hidden_in, cotangent, quarter, rows, chips), "chip")
    given = swap(own, "core", 1)

    small = low_rank_parts(index, hidden_in, gains, down, up, quarter, sections)
    small = exchange(small, "section")

    source = SPREAD // rows
    blocks = exchange(block, fsdp)
    mixing = exchange(mixing_copies(blocks[:source], sections, source), "section")

    mine, other = partial_products(own, given, weights, rows)
    pieces = exchange(sum_cores(mine, swap(other, "core", 1)), "chip")
    sums = exchange(sum_chips(index, pieces, small), "chip")
    other_sums = swap(sums, "core", 1)

    grown, grads = chain(
        index, sums, other_sums, own, given, mixing, small, weights, rows, width
    )

    gradient = jnp.sum(exchange(grads, "section").astype(f32), axis=0)
    per = value_width // devices
    gain_here = lax.dynamic_slice_in_dim(gains[0].astype(f32), j * rows, rows)
    down_grad = (gradient[:, :rows] * gain_here[None, :]).T
    up_grad = lax.dynamic_slice_in_dim(gradient[:, rows:], j * per, per, 1).T

    moved = grown.reshape(sections * devices, quarter, rows)
    moved = exchange(moved, ("section", "chip", "core"))
    input_grad = placed(moved.reshape(sections, devices, quarter, rows), cotangent)
    return (input_grad, down_grad[None], up_grad[None])


def solution(mesh):
    sections, devices = mesh.devices.shape
    split = jax.sharding.Mesh(
        mesh.devices.reshape(sections, devices // 2, 2), ("section", "chip", "core")
    )
    fsdp = ("chip", "core")
    return jax.shard_map(
        shards,
        mesh=split,
        in_specs=(
            P("section", fsdp, None),
            P("section", fsdp, None),
            P("section", fsdp),
            P("section", None),
            P("section", None, None),
            P("section", None, None),
            P(fsdp, None),
            P(fsdp, None),
        ),
        out_specs=(
            P("section", fsdp, None),
            P("section", fsdp, None),
            P("section", fsdp, None),
        ),
        check_vma=False,
    )
```

```python
import jax
import jax.numpy as jnp
from jax import lax
from jax.experimental import pallas as pl
from jax.experimental.pallas import tpu as pltpu
from jax.sharding import PartitionSpec as P

HEAD = 128
GROUP = 8
KV_HEADS = 4
BLOCK = 64
SROWS = 32
SPREAD = KV_HEADS * GROUP * HEAD

NF4_TABLE = (
    -1.0,
    -0.6961928009986877,
    -0.5250730514526367,
    -0.39491748809814453,
    -0.28444138169288635,
    -0.18477343022823334,
    -0.09105003625154495,
    0.0,
    0.07958029955625534,
    0.16093020141124725,
    0.24611230194568634,
    0.33791524171066284,
    0.44070982933044434,
    0.5626170039176941,
    0.7229568362236023,
    1.0,
)
adapter_scale = 0.5
epsilon = 1e-05
f32 = jnp.float32
bf16 = jnp.bfloat16


def swap(block, axis, distance):
    size = lax.axis_size(axis)
    return lax.ppermute(block, axis, [(i, i ^ distance) for i in range(size)])


def exchange(blocks, axis):
    return lax.all_to_all(blocks, axis, 0, 0, tiled=True)


def forwarded(halves, axis):
    size = lax.axis_size(axis)
    first, second = {0: halves[0]}, {0: halves[1]}
    for hops in range(1, size.bit_length()):
        for d in range(1, size):
            if d.bit_count() == hops:
                high, low = 1 << (d.bit_length() - 1), d & -d
                first[d] = swap(first[d ^ high], axis, high)
                second[d] = swap(second[d ^ low], axis, low)
    return [(first[d], second[d]) for d in range(size)]


def product(a, b):
    return jnp.dot(a, b, preferred_element_type=f32)


def product_bt(a, b):
    return lax.dot_general(a, b, (((1,), (1,)), ((), ())), preferred_element_type=f32)


def product_at(a, b):
    return lax.dot_general(a, b, (((0,), (0,)), ((), ())), preferred_element_type=f32)


def looked_up(codes):
    values = [f32(v) for v in NF4_TABLE]
    bit = 1
    while len(values) > 1:
        odd = (codes & bit) != 0
        values = [jnp.where(odd, values[i + 1], values[i]) for i in range(0, len(values), 2)]
        bit *= 2
    return values[0]


def effective_rows(index, codes, scale_codes, second_scales, gains, down, up):
    rows, width = codes.shape[1:]
    rank = down.shape[1]
    step = min(256, rows // 2)
    steps = rows // step
    scales = width // BLOCK

    def kernel(index_ref, code_ref, scale_ref, second_ref, gain_ref, down_ref, up_ref,
               first_ref, last_ref, mix_ref, acc_ref):
        i = pl.program_id(0)
        lane = lax.broadcasted_iota(jnp.int32, (1, step), 1) // SROWS
        second = jnp.zeros((1, step), f32)
        for g in range(step // SROWS):
            second = jnp.where(lane == g, second_ref[0, i * (step // SROWS) + g], second)
        gain = gain_ref[...].astype(f32)
        factor = second * (scale_ref[0].astype(f32) + 1.0) / 256.0 * gain
        near = factor.astype(bf16)
        rest = (factor - near.astype(f32)).astype(bf16)
        at_block = lax.broadcasted_iota(jnp.int32, (2 * scales, width), 1) // BLOCK
        row = lax.broadcasted_iota(jnp.int32, (2 * scales, width), 0) % scales
        expand = jnp.where(at_block == row, 1.0, 0.0).astype(bf16)
        wide = product_at(jnp.concatenate([near, rest], axis=0), expand)
        gained = (gain * adapter_scale * down_ref[0].astype(f32)).astype(bf16)
        low = product_at(gained, up_ref[0])
        made = (looked_up(code_ref[0]) * wide + low).astype(bf16)

        @pl.when(i < steps // 2)
        def _():
            first_ref[...] = made

        @pl.when(i >= steps // 2)
        def _():
            last_ref[...] = made

        mixed = jnp.sum(made.astype(f32).reshape(step // HEAD, HEAD, width), axis=0)

        @pl.when(i == 0)
        def _():
            acc_ref[...] = mixed

        @pl.when(i > 0)
        def _():
            acc_ref[...] += mixed

        @pl.when(i == steps - 1)
        def _():
            mix_ref[...] = acc_ref[...].astype(bf16)

    half = steps // 2
    return pl.pallas_call(
        kernel,
        grid_spec=pltpu.PrefetchScalarGridSpec(
            num_scalar_prefetch=1,
            grid=(steps,),
            in_specs=[
                pl.BlockSpec((1, step, width), lambda i, ix: (0, i, 0)),
                pl.BlockSpec((1, scales, step), lambda i, ix: (0, 0, i)),
                pl.BlockSpec(memory_space=pltpu.SMEM),
                pl.BlockSpec((1, step), lambda i, ix: (0, ix[1] * steps + i)),
                pl.BlockSpec((1, rank, step), lambda i, ix: (0, 0, ix[1] * steps + i)),
                pl.BlockSpec((1, rank, width), lambda i, ix: (0, 0, 0)),
            ],
            out_specs=[
                pl.BlockSpec((step, width), lambda i, ix: (jnp.minimum(i, half - 1), 0)),
                pl.BlockSpec((step, width), lambda i, ix: (jnp.maximum(i - half, 0), 0)),
                pl.BlockSpec((HEAD, width), lambda i, ix: (0, 0)),
            ],
            scratch_shapes=[pltpu.VMEM((HEAD, width), f32)],
        ),
        out_shape=(
            jax.ShapeDtypeStruct((rows // 2, width), bf16),
            jax.ShapeDtypeStruct((rows // 2, width), bf16),
            jax.ShapeDtypeStruct((HEAD, width), bf16),
        ),
        name="effective_rows",
    )(index, codes, scale_codes, second_scales, gains, down, up)


def hidden_parts(index, hidden, cotangent, block, quarter, rows, chips):
    width = hidden.shape[1]
    value_width = KV_HEADS * HEAD
    tail_end = 2 * rows + 3 * value_width + HEAD
    folds = HEAD // quarter
    total = tail_end + folds * value_width

    def kernel(index_ref, h_ref, c_ref, b_ref, out_ref):
        core = index_ref[1] % 2
        hidden_rows = h_ref[...].astype(f32)
        square = jnp.sum(hidden_rows * hidden_rows, axis=1, keepdims=True)
        high = square.astype(bf16).astype(f32)
        middle = (square - high).astype(bf16).astype(f32)
        lane = lax.broadcasted_iota(jnp.int32, (quarter, HEAD), 1)
        squares = jnp.where(lane == 0, high, jnp.where(lane == 1, middle, square - high - middle))
        squares = jnp.where(lane < 3, squares, 0.0).astype(bf16)
        tails = [[], [], []]
        for k in range(KV_HEADS):
            ch = jnp.zeros((quarter, HEAD), f32)
            cc = jnp.zeros((quarter, HEAD), f32)
            for g in range(GROUP):
                at = slice((k * GROUP + g) * HEAD, (k * GROUP + g + 1) * HEAD)
                ch = ch + hidden_rows[:, at]
                cc = cc + c_ref[:, at].astype(f32)
            near = ch.astype(bf16)
            tails[0].append(near)
            tails[1].append((ch - near.astype(f32)).astype(bf16))
            tails[2].append(cc.astype(bf16))
        tail = jnp.concatenate(tails[0] + tails[1] + tails[2] + [squares], axis=1)
        for z in range(chips):
            keep = pl.multiple_of((2 * z + core) * rows, HEAD)
            give = pl.multiple_of((2 * z + 1 - core) * rows, HEAD)
            out_ref[z, :, :rows] = h_ref[:, pl.ds(keep, rows)]
            out_ref[z, :, rows : 2 * rows] = h_ref[:, pl.ds(give, rows)]
            out_ref[z, :, 2 * rows : tail_end] = tail
            for i in range(folds):
                at = tail_end + i * value_width
                out_ref[z, :, at : at + value_width] = b_ref[i * quarter : (i + 1) * quarter]

    return pl.pallas_call(
        kernel,
        grid_spec=pltpu.PrefetchScalarGridSpec(
            num_scalar_prefetch=1,
            grid=(1,),
            in_specs=[
                pl.BlockSpec((quarter, width), lambda i, ix: (ix[0], 0)),
                pl.BlockSpec((quarter, SPREAD), lambda i, ix: (ix[0], 0)),
                pl.BlockSpec((HEAD, value_width), lambda i, ix: (0, 0)),
            ],
            out_specs=pl.BlockSpec((chips, quarter, total), lambda i, ix: (0, 0, 0)),
        ),
        out_shape=jax.ShapeDtypeStruct((chips, quarter, total), bf16),
        name="hidden_parts",
    )(index, hidden, cotangent, block)


def low_rank_parts(index, hidden, gains, down, up, quarter, sections):
    count, width = hidden.shape
    rank = down.shape[1]
    value_width = up.shape[2]
    chunk = GROUP * HEAD

    def kernel(index_ref, h_ref, gain_ref, down_ref, up_ref, *refs):
        outs, low_ref = refs[:-1], refs[-1]
        low = jnp.zeros((count, rank), f32)
        mixes = []
        for k in range(width // chunk):
            at = slice(k * chunk, (k + 1) * chunk)
            gained = (gain_ref[:, at].astype(f32) * down_ref[0, :, at].astype(f32)).astype(bf16)
            low = low + product_bt(h_ref[:, at], gained)
            if k < KV_HEADS:
                parts = [gained[:, g * HEAD : (g + 1) * HEAD].astype(f32) for g in range(GROUP)]
                mixes.append(sum(parts[1:], parts[0]))
        mixed = jnp.concatenate(mixes, axis=1).astype(bf16)
        low = jnp.concatenate([low, jnp.zeros((count, value_width - rank), f32)], axis=1)
        low_ref[...] = low
        for d in range(sections):
            start = pl.multiple_of((index_ref[0] ^ d) * quarter, quarter)
            outs[d][:rank] = mixed
            outs[d][rank : 2 * rank] = up_ref[0]
            outs[d][2 * rank :] = low_ref[pl.ds(start, quarter)].astype(bf16)

    vmem = pl.BlockSpec(memory_space=pltpu.VMEM)
    return pl.pallas_call(
        kernel,
        in_specs=[pl.BlockSpec(memory_space=pltpu.SMEM)] + [vmem] * 4,
        out_shape=[jax.ShapeDtypeStruct((2 * rank + quarter, value_width), bf16)] * sections,
        scratch_shapes=[pltpu.VMEM((count, value_width), f32)],
        name="low_rank_parts",
    )(index, hidden, gains, down, up)


def mixing_matrix(index, own, given, quarter, source):
    value_width = KV_HEADS * HEAD
    folds = HEAD // quarter
    start = own.shape[2] - folds * value_width
    each = source // KV_HEADS

    def kernel(index_ref, own_ref, given_ref, out_ref):
        even = index_ref[1] % 2 == 0
        for k in range(KV_HEADS):
            for i in range(folds):
                at = slice(start + i * value_width, start + (i + 1) * value_width)
                made = jnp.zeros((quarter, value_width), f32)
                for j in range(k * each, (k + 1) * each):
                    mine = even if j % 2 == 0 else jnp.logical_not(even)
                    came = jnp.where(mine, own_ref[j // 2, :, at], given_ref[j // 2, :, at])
                    made = made + came.astype(f32)
                row = k * HEAD + i * quarter
                out_ref[row : row + quarter] = made.astype(bf16)

    vmem = pl.BlockSpec(memory_space=pltpu.VMEM)
    return pl.pallas_call(
        kernel,
        in_specs=[pl.BlockSpec(memory_space=pltpu.SMEM), vmem, vmem],
        out_shape=jax.ShapeDtypeStruct((value_width, value_width), bf16),
        name="mixing_matrix",
    )(index, own, given)


def partial_products(own, given, weights, rows):
    chips, quarter = own.shape[:2]
    sections = len(weights)
    width = weights[0][0].shape[1]
    half = rows // 2
    tokens = chips * quarter

    def kernel(*refs):
        own_ref, given_ref = refs[:2]
        weight_refs = refs[2:-2]
        left = own_ref[:, :, :rows].reshape(tokens, rows)
        right = given_ref[:, :, rows : 2 * rows].reshape(tokens, rows)
        both = jnp.concatenate([left, right], axis=0)
        for d in range(sections):
            made = product(both[:, :half], weight_refs[2 * d][...])
            made = made + product(both[:, half:], weight_refs[2 * d + 1][...])
            made = made.astype(bf16).reshape(2, chips, quarter, width)
            refs[-2][:, d] = made[0]
            refs[-1][:, d] = made[1]

    shape = jax.ShapeDtypeStruct((chips, sections, quarter, width), bf16)
    flat = [piece for pair in weights for piece in pair]
    return pl.pallas_call(kernel, out_shape=(shape, shape), name="partials")(own, given, *flat)


def sum_cores(mine, other):
    def kernel(a_ref, b_ref, out_ref):
        out_ref[...] = (a_ref[...].astype(f32) + b_ref[...].astype(f32)).astype(bf16)

    return pl.pallas_call(
        kernel, out_shape=jax.ShapeDtypeStruct(mine.shape, bf16), name="sum_cores"
    )(mine, other)


def sum_chips(pieces, smalls):
    chips, sections, quarter, width = pieces.shape
    skip = smalls[0].shape[0] - quarter

    def kernel(p_ref, *refs):
        total = p_ref[0].astype(f32)
        for z in range(1, chips):
            total = total + p_ref[z].astype(f32)
        total = total.astype(bf16)
        for z in range(chips):
            refs[-1][z, :, :, :width] = total
            for d in range(sections):
                refs[-1][z, d, :, width:] = refs[d][skip:, :HEAD]

    return pl.pallas_call(
        kernel,
        out_shape=jax.ShapeDtypeStruct((chips, sections, quarter, width + HEAD), bf16),
        name="sum_chips",
    )(pieces, *smalls)


def chain(index, sums, other_sums, own, given, mixings, smalls, weights, rows, width):
    chips, sections, quarter, _ = sums.shape
    value_width = mixings[0].shape[1]
    rank = HEAD // 2
    tail_end = 2 * rows + 3 * value_width + HEAD
    tokens = 2 * chips * quarter
    groups = rows // HEAD
    half = rows // 2

    def kernel(index_ref, *refs):
        refs = list(refs)
        take = lambda n: [refs.pop(0) for _ in range(n)]
        sum_ref, other_ref, own_ref, given_ref = take(4)
        mix_in, small_in, weight_in = take(sections), take(sections), take(2 * sections)
        (out_ref,) = take(1)
        grad_refs = take(sections)
        v_ref, mix_ref, small_ref, w_ref, grad_ref, sems = take(6)
        me = index_ref[0]
        core = index_ref[1] % 2
        head = index_ref[2]
        early, copies = [], []
        for d in range(sections):
            early.append(pltpu.make_async_copy(mix_in[d], mix_ref.at[me ^ d], sems.at[2, d]))
            early.append(
                pltpu.make_async_copy(
                    small_in[d].at[pl.ds(0, 2 * rank)], small_ref.at[me ^ d], sems.at[3, d]
                )
            )
        for copy in early:
            copy.start()
        for d in range(sections):
            for p in range(2):
                copies.append(
                    pltpu.make_async_copy(
                        weight_in[2 * d + p],
                        w_ref.at[me ^ d, pl.ds(p * half, half)],
                        sems.at[p, d],
                    )
                )
        for copy in copies:
            copy.start()

        def both(left, right):
            merged = jnp.concatenate([left, right], axis=0)
            return merged.reshape(tokens, merged.shape[-1])

        tail = both(own_ref[:, :, 2 * rows : tail_end], given_ref[:, :, 2 * rows : tail_end])
        hx = both(own_ref[:, :, :rows], given_ref[:, :, rows : 2 * rows]).astype(f32)
        ch = tail[:, :value_width].astype(f32) + tail[:, value_width : 2 * value_width].astype(f32)
        sq = jnp.sum(tail[:, 3 * value_width :].astype(f32), axis=1, keepdims=True)
        for copy in early:
            copy.wait()
        total = jnp.zeros((tokens, value_width), f32)
        before, inverse, lows = [], [], []
        for m in range(sections):
            d = me ^ m
            rm2 = (
                sq
                + 2.0 * jnp.sum(total * ch, axis=1, keepdims=True)
                + GROUP * jnp.sum(total * total, axis=1, keepdims=True)
            ) / width + epsilon
            r = lax.rsqrt(rm2)
            start = both(sum_ref[:, d], other_ref[:, d]).astype(f32)
            rounded = total.astype(bf16)
            v = (start[:, :value_width] + product(rounded, mix_ref[m])) * r
            low = start[:, value_width : value_width + rank]
            low = low + product_bt(rounded, small_ref[m, :rank])
            v_ref[m] = v
            lows.append((low * r).astype(bf16))
            before.append(rounded)
            inverse.append(r)
            total = total + v
        for copy in copies:
            copy.wait()
        direction = tail[:, 2 * value_width : 3 * value_width].astype(f32)
        grown = jnp.zeros((tokens, rows), f32)
        for m in reversed(range(sections)):
            r = inverse[m]
            rounded = direction.astype(bf16)
            mean = jnp.sum(rounded.astype(f32) * v_ref[m], axis=1, keepdims=True) / width
            q = mean * r * r
            scaled = (direction * r).astype(bf16)
            low_grad = adapter_scale * product_bt(rounded, small_ref[m, rank : 2 * rank]) * r
            grad_ref[m, :, rows:] = (adapter_scale * product_at(lows[m], rounded)).astype(bf16)
            earlier = before[m].astype(f32)
            spread = jnp.zeros((tokens, HEAD), f32)
            for k in range(KV_HEADS):
                spread = spread + jnp.where(head == k, earlier[:, k * HEAD : (k + 1) * HEAD], 0.0)
            hidden = hx + jnp.concatenate([spread] * groups, axis=1)
            grad_ref[m, :, :rows] = product_at(
                low_grad.astype(bf16), hidden.astype(bf16)
            ).astype(bf16)
            grown = grown + product_bt(scaled, w_ref[m]) - hidden * q
            out = grown.astype(bf16).reshape(2, chips, quarter, rows)
            for e in range(2):
                for z in range(chips):
                    out_ref[m, 2 * z + (core ^ e)] = out[e, z]
            direction = direction + product_bt(scaled, mix_ref[m]) - (ch + GROUP * earlier) * q
        for d in range(sections):
            grad_refs[d][...] = grad_ref[me ^ d]

    vmem = pl.BlockSpec(memory_space=pltpu.VMEM)
    anywhere = pl.BlockSpec(memory_space=pl.ANY)
    flat = [piece for pair in weights for piece in pair]
    grad_width = rows + value_width
    outs = pl.pallas_call(
        kernel,
        in_specs=[pl.BlockSpec(memory_space=pltpu.SMEM)]
        + [vmem] * 4
        + [anywhere] * (4 * sections),
        out_shape=[jax.ShapeDtypeStruct((sections, 2 * chips, quarter, rows), bf16)]
        + [jax.ShapeDtypeStruct((rank, grad_width), bf16)] * sections,
        scratch_shapes=[
            pltpu.VMEM((sections, tokens, value_width), f32),
            pltpu.VMEM((sections, value_width, value_width), bf16),
            pltpu.VMEM((sections, 2 * rank, value_width), bf16),
            pltpu.VMEM((sections, rows, value_width), bf16),
            pltpu.VMEM((sections, rank, grad_width), bf16),
            pltpu.SemaphoreType.DMA((4, sections)),
        ],
        name="chain",
    )(index, sums, other_sums, own, given, *mixings, *smalls, *flat)
    return outs[0], outs[1:]


def placed(moved, cotangent):
    sections, devices, quarter, rows = moved.shape
    count, width = cotangent.shape

    def kernel(m_ref, c_ref, out_ref):
        for j in range(devices):
            at = slice(j * rows, (j + 1) * rows)
            out_ref[0, :, at] = (c_ref[:, at].astype(f32) + m_ref[0, j].astype(f32)).astype(bf16)

    return pl.pallas_call(
        kernel,
        grid=(sections,),
        in_specs=[
            pl.BlockSpec((1, devices, quarter, rows), lambda i: (i, 0, 0, 0)),
            pl.BlockSpec((quarter, width), lambda i: (i, 0)),
        ],
        out_specs=pl.BlockSpec((1, quarter, width), lambda i: (0, i, 0)),
        out_shape=jax.ShapeDtypeStruct((1, count, width), bf16),
        name="placed",
    )(moved, cotangent)


def layers(
    codes,
    scale_codes,
    second_scales,
    gains,
    down_adapter,
    up_projection_weight,
    hidden_in,
    cotangent,
):
    fsdp = ("chip", "core")
    s = lax.axis_index("section")
    j = lax.axis_index(fsdp)
    sections = lax.axis_size("section")
    chips = lax.axis_size("chip")
    devices = lax.axis_size(fsdp)
    count, width = hidden_in.shape
    quarter = count // sections
    rows, value_width = codes.shape[1], codes.shape[2]
    index = jnp.stack([s, j, j * rows // (GROUP * HEAD)]).astype(jnp.int32)
    scale_codes = jnp.swapaxes(scale_codes, 1, 2)
    down = jnp.swapaxes(down_adapter, 1, 2)
    up = jnp.swapaxes(up_projection_weight, 1, 2)

    first, second, block = effective_rows(
        index, codes, scale_codes, second_scales, gains, down, up
    )
    weights = forwarded((first, second), "section")

    own = hidden_parts(index, hidden_in, cotangent, block, quarter, rows, chips)
    own = exchange(own, "chip")
    given = swap(own, "core", 1)

    smalls = list(low_rank_parts(index, hidden_in, gains, down, up, quarter, sections))
    for d in range(1, sections):
        smalls[d] = swap(smalls[d], "section", d)

    mixing = mixing_matrix(index, own, given, quarter, SPREAD // rows)
    mixings = [mixing]
    for d in range(1, sections):
        mixings.append(swap(mixing, "section", d))

    mine, other = partial_products(own, given, weights, rows)
    pieces = exchange(sum_cores(mine, swap(other, "core", 1)), "chip")
    sums = exchange(sum_chips(pieces, smalls), "chip")
    other_sums = swap(sums, "core", 1)

    grown, grads = chain(
        index, sums, other_sums, own, given, mixings, smalls, weights, rows, width
    )

    gradient = grads[0].astype(f32)
    for d in range(1, sections):
        gradient = gradient + swap(grads[d], "section", d).astype(f32)
    per = value_width // devices
    gain_here = lax.dynamic_slice_in_dim(gains[0].astype(f32), j * rows, rows)
    down_grad = (gradient[:, :rows] * gain_here[None, :]).T
    up_grad = lax.dynamic_slice_in_dim(gradient[:, rows:], j * per, per, 1).T

    moved = grown.reshape(sections * devices, quarter, rows)
    moved = exchange(moved, ("section", "chip", "core"))
    input_grad = placed(moved.reshape(sections, devices, quarter, rows), cotangent)
    return (input_grad, down_grad[None], up_grad[None])


def solution(mesh):
    sections, devices = mesh.devices.shape
    split = jax.sharding.Mesh(
        mesh.devices.reshape(sections, devices // 2, 2), ("section", "chip", "core")
    )
    fsdp = ("chip", "core")
    return jax.shard_map(
        layers,
        mesh=split,
        in_specs=(
            P("section", fsdp, None),
            P("section", fsdp, None),
            P("section", fsdp),
            P("section", None),
            P("section", None, None),
            P("section", None, None),
            P(fsdp, None),
            P(fsdp, None),
        ),
        out_specs=(
            P("section", fsdp, None),
            P("section", fsdp, None),
            P("section", fsdp, None),
        ),
        check_vma=False,
    )
```

```python
import jax
import jax.numpy as jnp
from jax import lax
from jax.experimental import pallas as pl
from jax.experimental.pallas import tpu as pltpu
from jax.sharding import PartitionSpec as P

HEAD = 128
GROUP = 8
KV_HEADS = 4
BLOCK = 64
SROWS = 32
SPREAD = KV_HEADS * GROUP * HEAD

NF4_TABLE = (
    -1.0,
    -0.6961928009986877,
    -0.5250730514526367,
    -0.39491748809814453,
    -0.28444138169288635,
    -0.18477343022823334,
    -0.09105003625154495,
    0.0,
    0.07958029955625534,
    0.16093020141124725,
    0.24611230194568634,
    0.33791524171066284,
    0.44070982933044434,
    0.5626170039176941,
    0.7229568362236023,
    1.0,
)
adapter_scale = 0.5
epsilon = 1e-05
f32 = jnp.float32


def room(mib):
    return pltpu.CompilerParams(vmem_limit_bytes=mib << 20)


bf16 = jnp.bfloat16


def swap(block, axis, distance):
    size = lax.axis_size(axis)
    return lax.ppermute(block, axis, [(i, i ^ distance) for i in range(size)])


def exchange(blocks, axis):
    return lax.all_to_all(blocks, axis, 0, 0, tiled=True)


def forwarded(halves, axis):
    size = lax.axis_size(axis)
    first, second = {0: halves[0]}, {0: halves[1]}
    for hops in range(1, size.bit_length()):
        for d in range(1, size):
            if d.bit_count() == hops:
                high, low = 1 << (d.bit_length() - 1), d & -d
                first[d] = swap(first[d ^ high], axis, high)
                second[d] = swap(second[d ^ low], axis, low)
    return [(first[d], second[d]) for d in range(size)]


def product(a, b):
    return jnp.dot(a, b, preferred_element_type=f32)


def product_bt(a, b):
    return lax.dot_general(a, b, (((1,), (1,)), ((), ())), preferred_element_type=f32)


def product_at(a, b):
    return lax.dot_general(a, b, (((0,), (0,)), ((), ())), preferred_element_type=f32)


def looked_up(codes):
    lane = lax.broadcasted_iota(jnp.int32, (codes.shape[0], HEAD), 1)
    table = jnp.zeros(lane.shape, f32)
    for entry, value in enumerate(NF4_TABLE):
        table = jnp.where(lane == entry, f32(value), table)
    parts = [
        jnp.take_along_axis(table, codes[:, at : at + HEAD], axis=1, mode="promise_in_bounds")
        for at in range(0, codes.shape[1], HEAD)
    ]
    return jnp.concatenate(parts, axis=1)


def effective_rows(index, codes, scale_codes, second_scales, gains, down, up):
    rows, width = codes.shape[1:]
    rank = down.shape[1]
    step = min(512, rows // 2)
    steps = rows // step
    scales = width // BLOCK

    def kernel(index_ref, code_ref, scale_ref, second_ref, gain_ref, down_ref, up_ref,
               first_ref, last_ref, mix_ref, acc_ref):
        i = pl.program_id(0)
        lane = lax.broadcasted_iota(jnp.int32, (1, step), 1) // SROWS
        second = jnp.zeros((1, step), f32)
        for g in range(step // SROWS):
            second = jnp.where(lane == g, second_ref[0, i * (step // SROWS) + g], second)
        gain = gain_ref[...].astype(f32)
        factor = second * (scale_ref[0].astype(f32) + 1.0) / 256.0 * gain
        near = factor.astype(bf16)
        rest = (factor - near.astype(f32)).astype(bf16)
        at_block = lax.broadcasted_iota(jnp.int32, (2 * scales, width), 1) // BLOCK
        row = lax.broadcasted_iota(jnp.int32, (2 * scales, width), 0) % scales
        expand = jnp.where(at_block == row, 1.0, 0.0).astype(bf16)
        wide = product_at(jnp.concatenate([near, rest], axis=0), expand)
        gained = (gain * adapter_scale * down_ref[0].astype(f32)).astype(bf16)
        low = product_at(gained, up_ref[0])
        made = (looked_up(code_ref[0]) * wide + low).astype(bf16)

        @pl.when(i < steps // 2)
        def _():
            first_ref[...] = made

        @pl.when(i >= steps // 2)
        def _():
            last_ref[...] = made

        mixed = jnp.sum(made.astype(f32).reshape(step // HEAD, HEAD, width), axis=0)

        @pl.when(i == 0)
        def _():
            acc_ref[...] = mixed

        @pl.when(i > 0)
        def _():
            acc_ref[...] += mixed

        @pl.when(i == steps - 1)
        def _():
            mix_ref[...] = acc_ref[...].astype(bf16)

    half = steps // 2
    return pl.pallas_call(
        kernel,
        grid_spec=pltpu.PrefetchScalarGridSpec(
            num_scalar_prefetch=1,
            grid=(steps,),
            in_specs=[
                pl.BlockSpec((1, step, width), lambda i, ix: (0, i, 0)),
                pl.BlockSpec((1, scales, step), lambda i, ix: (0, 0, i)),
                pl.BlockSpec(memory_space=pltpu.SMEM),
                pl.BlockSpec((1, step), lambda i, ix: (0, ix[1] * steps + i)),
                pl.BlockSpec((1, rank, step), lambda i, ix: (0, 0, ix[1] * steps + i)),
                pl.BlockSpec((1, rank, width), lambda i, ix: (0, 0, 0)),
            ],
            out_specs=[
                pl.BlockSpec((step, width), lambda i, ix: (jnp.minimum(i, half - 1), 0)),
                pl.BlockSpec((step, width), lambda i, ix: (jnp.maximum(i - half, 0), 0)),
                pl.BlockSpec((HEAD, width), lambda i, ix: (0, 0)),
            ],
            scratch_shapes=[pltpu.VMEM((HEAD, width), f32)],
        ),
        out_shape=(
            jax.ShapeDtypeStruct((rows // 2, width), bf16),
            jax.ShapeDtypeStruct((rows // 2, width), bf16),
            jax.ShapeDtypeStruct((HEAD, width), bf16),
        ),
        name="effective_rows",
    )(index, codes, scale_codes, second_scales, gains, down, up)


def hidden_parts(index, hidden, cotangent, block, quarter, rows, chips):
    width = hidden.shape[1]
    value_width = KV_HEADS * HEAD
    tail_end = 3 * value_width + HEAD
    folds = HEAD // quarter
    total = tail_end + folds * value_width

    def kernel(index_ref, h_ref, c_ref, b_ref, out_ref, tail_ref):
        core = index_ref[1] % 2
        hidden_rows = h_ref[...].astype(f32)
        square = jnp.sum(hidden_rows * hidden_rows, axis=1, keepdims=True)
        high = square.astype(bf16).astype(f32)
        middle = (square - high).astype(bf16).astype(f32)
        lane = lax.broadcasted_iota(jnp.int32, (quarter, HEAD), 1)
        squares = jnp.where(lane == 0, high, jnp.where(lane == 1, middle, square - high - middle))
        squares = jnp.where(lane < 3, squares, 0.0).astype(bf16)
        tails = [[], [], []]
        for k in range(KV_HEADS):
            ch = jnp.zeros((quarter, HEAD), f32)
            cc = jnp.zeros((quarter, HEAD), f32)
            for g in range(GROUP):
                at = slice((k * GROUP + g) * HEAD, (k * GROUP + g + 1) * HEAD)
                ch = ch + hidden_rows[:, at]
                cc = cc + c_ref[:, at].astype(f32)
            near = ch.astype(bf16)
            tails[0].append(near)
            tails[1].append((ch - near.astype(f32)).astype(bf16))
            tails[2].append(cc.astype(bf16))
        tail = jnp.concatenate(tails[0] + tails[1] + tails[2] + [squares], axis=1)
        for z in range(chips):
            keep = pl.multiple_of((2 * z + core) * rows, HEAD)
            give = pl.multiple_of((2 * z + 1 - core) * rows, HEAD)
            out_ref[z, :, :rows] = h_ref[:, pl.ds(keep, rows)]
            out_ref[z, :, rows : 2 * rows] = h_ref[:, pl.ds(give, rows)]
        tail_ref[:, :tail_end] = tail
        for i in range(folds):
            at = tail_end + i * value_width
            tail_ref[:, at : at + value_width] = b_ref[i * quarter : (i + 1) * quarter]

    return pl.pallas_call(
        kernel,
        grid_spec=pltpu.PrefetchScalarGridSpec(
            num_scalar_prefetch=1,
            grid=(1,),
            in_specs=[
                pl.BlockSpec((quarter, width), lambda i, ix: (ix[0], 0)),
                pl.BlockSpec((quarter, SPREAD), lambda i, ix: (ix[0], 0)),
                pl.BlockSpec((HEAD, value_width), lambda i, ix: (0, 0)),
            ],
            out_specs=[
                pl.BlockSpec((chips, quarter, 2 * rows), lambda i, ix: (0, 0, 0)),
                pl.BlockSpec((quarter, total), lambda i, ix: (0, 0)),
            ],
        ),
        out_shape=(
            jax.ShapeDtypeStruct((chips, quarter, 2 * rows), bf16),
            jax.ShapeDtypeStruct((quarter, total), bf16),
        ),
        name="hidden_parts",
    )(index, hidden, cotangent, block)


def low_rank_parts(index, hidden, gains, down, up, quarter, sections):
    count, width = hidden.shape
    rank = down.shape[1]
    value_width = up.shape[2]
    chunk = GROUP * HEAD

    def kernel(index_ref, h_ref, gain_ref, down_ref, up_ref, *refs):
        outs, low_ref = refs[:-1], refs[-1]
        low = jnp.zeros((count, rank), f32)
        mixes = []
        for k in range(width // chunk):
            at = slice(k * chunk, (k + 1) * chunk)
            gained = (gain_ref[:, at].astype(f32) * down_ref[0, :, at].astype(f32)).astype(bf16)
            low = low + product_bt(h_ref[:, at], gained)
            if k < KV_HEADS:
                parts = [gained[:, g * HEAD : (g + 1) * HEAD].astype(f32) for g in range(GROUP)]
                mixes.append(sum(parts[1:], parts[0]))
        mixed = jnp.concatenate(mixes, axis=1).astype(bf16)
        low = jnp.concatenate([low, jnp.zeros((count, value_width - rank), f32)], axis=1)
        low_ref[...] = low
        for d in range(sections):
            start = pl.multiple_of((index_ref[0] ^ d) * quarter, quarter)
            outs[d][:rank] = mixed
            outs[d][rank : 2 * rank] = up_ref[0]
            outs[d][2 * rank :] = low_ref[pl.ds(start, quarter)].astype(bf16)

    vmem = pl.BlockSpec(memory_space=pltpu.VMEM)
    return pl.pallas_call(
        kernel,
        in_specs=[pl.BlockSpec(memory_space=pltpu.SMEM)] + [vmem] * 4,
        out_shape=[jax.ShapeDtypeStruct((2 * rank + quarter, value_width), bf16)] * sections,
        scratch_shapes=[pltpu.VMEM((count, value_width), f32)],
        name="low_rank_parts",
    )(index, hidden, gains, down, up)


def in_chip_order(index, tails):
    def kernel(index_ref, *refs):
        z = index_ref[1] // 2
        for d in range(len(tails)):
            refs[-1][z ^ d] = refs[d][...]

    vmem = pl.BlockSpec(memory_space=pltpu.VMEM)
    return pl.pallas_call(
        kernel,
        in_specs=[pl.BlockSpec(memory_space=pltpu.SMEM)] + [vmem] * len(tails),
        out_shape=jax.ShapeDtypeStruct((len(tails),) + tails[0].shape, bf16),
        compiler_params=room(6),
        name="in_chip_order",
    )(index, *tails)


def mixing_matrix(index, own, given, quarter, source):
    value_width = KV_HEADS * HEAD
    folds = HEAD // quarter
    start = own.shape[2] - folds * value_width
    each = source // KV_HEADS

    def kernel(index_ref, own_ref, given_ref, out_ref):
        even = index_ref[1] % 2 == 0
        for k in range(KV_HEADS):
            for i in range(folds):
                at = slice(start + i * value_width, start + (i + 1) * value_width)
                made = jnp.zeros((quarter, value_width), f32)
                for j in range(k * each, (k + 1) * each):
                    mine = even if j % 2 == 0 else jnp.logical_not(even)
                    came = jnp.where(mine, own_ref[j // 2, :, at], given_ref[j // 2, :, at])
                    made = made + came.astype(f32)
                row = k * HEAD + i * quarter
                out_ref[row : row + quarter] = made.astype(bf16)

    vmem = pl.BlockSpec(memory_space=pltpu.VMEM)
    return pl.pallas_call(
        kernel,
        in_specs=[pl.BlockSpec(memory_space=pltpu.SMEM), vmem, vmem],
        out_shape=jax.ShapeDtypeStruct((value_width, value_width), bf16),
        compiler_params=room(6),
        name="mixing_matrix",
    )(index, own, given)


def partial_products(own, given, weights, rows):
    chips, quarter = own.shape[:2]
    sections = len(weights)
    width = weights[0][0].shape[1]
    half = rows // 2
    tokens = chips * quarter

    def kernel(*refs):
        own_ref, given_ref = refs[:2]
        weight_refs = refs[2:-2]
        left = own_ref[:, :, :rows].reshape(tokens, rows)
        right = given_ref[...].reshape(tokens, rows)
        both = jnp.concatenate([left, right], axis=0)
        for d in range(sections):
            made = product(both[:, :half], weight_refs[2 * d][...])
            made = made + product(both[:, half:], weight_refs[2 * d + 1][...])
            made = made.astype(bf16).reshape(2, chips, quarter, width)
            refs[-2][:, d] = made[0]
            refs[-1][:, d] = made[1]

    shape = jax.ShapeDtypeStruct((chips, sections, quarter, width), bf16)
    flat = [piece for pair in weights for piece in pair]
    return pl.pallas_call(
        kernel, out_shape=(shape, shape), compiler_params=room(16), name="partials"
    )(own, given, *flat)


def sum_cores(mine, other):
    def kernel(a_ref, b_ref, out_ref):
        out_ref[...] = (a_ref[...].astype(f32) + b_ref[...].astype(f32)).astype(bf16)

    return pl.pallas_call(
        kernel,
        out_shape=jax.ShapeDtypeStruct(mine.shape, bf16),
        compiler_params=room(6),
        name="sum_cores",
    )(mine, other)


def sum_chips(pieces, smalls):
    chips, sections, quarter, width = pieces.shape
    skip = smalls[0].shape[0] - quarter

    def kernel(p_ref, *refs):
        total = p_ref[0].astype(f32)
        for z in range(1, chips):
            total = total + p_ref[z].astype(f32)
        total = total.astype(bf16)
        for z in range(chips):
            refs[-1][z, :, :, :width] = total
            for d in range(sections):
                refs[-1][z, d, :, width:] = refs[d][skip:, :HEAD]

    return pl.pallas_call(
        kernel,
        out_shape=jax.ShapeDtypeStruct((chips, sections, quarter, width + HEAD), bf16),
        compiler_params=room(6),
        name="sum_chips",
    )(pieces, *smalls)


def chain(index, sums, other_sums, own, given, tails, mixings, smalls, weights, rows, width):
    chips, sections, quarter, _ = sums.shape
    value_width = mixings[0].shape[1]
    rank = HEAD // 2
    tail_end = 3 * value_width + HEAD
    tokens = 2 * chips * quarter
    groups = rows // HEAD
    half = rows // 2

    def kernel(index_ref, *refs):
        refs = list(refs)
        take = lambda n: [refs.pop(0) for _ in range(n)]
        sum_ref, other_ref, own_ref, given_ref, tail_ref, far_ref = take(6)
        mix_in, small_in, weight_in = take(sections), take(sections), take(2 * sections)
        (out_hbm,) = take(1)
        grad_refs = take(sections)
        out_ref, v_ref, mix_ref, small_ref, w_ref, grad_ref, sems = take(7)
        me = index_ref[0]
        core = index_ref[1] % 2
        head = index_ref[2]
        early, copies = [], []
        for d in range(sections):
            early.append(pltpu.make_async_copy(mix_in[d], mix_ref.at[me ^ d], sems.at[2, d]))
            early.append(
                pltpu.make_async_copy(
                    small_in[d].at[pl.ds(0, 2 * rank)], small_ref.at[me ^ d], sems.at[3, d]
                )
            )
        for copy in early:
            copy.start()
        for d in range(sections):
            for p in range(2):
                copies.append(
                    pltpu.make_async_copy(
                        weight_in[2 * d + p],
                        w_ref.at[me ^ d, pl.ds(p * half, half)],
                        sems.at[p, d],
                    )
                )
        for copy in copies:
            copy.start()

        def both(left, right):
            merged = jnp.concatenate([left, right], axis=0)
            return merged.reshape(tokens, merged.shape[-1])

        tail = both(tail_ref[:, :, :tail_end], far_ref[:, :, :tail_end])
        hx = both(own_ref[:, :, :rows], given_ref[...]).astype(f32)
        ch = tail[:, :value_width].astype(f32) + tail[:, value_width : 2 * value_width].astype(f32)
        sq = jnp.sum(tail[:, 3 * value_width :].astype(f32), axis=1, keepdims=True)
        for copy in early:
            copy.wait()
        total = jnp.zeros((tokens, value_width), f32)
        before, inverse, lows = [], [], []
        for m in range(sections):
            d = me ^ m
            rm2 = (
                sq
                + 2.0 * jnp.sum(total * ch, axis=1, keepdims=True)
                + GROUP * jnp.sum(total * total, axis=1, keepdims=True)
            ) / width + epsilon
            r = lax.rsqrt(rm2)
            start = both(sum_ref[:, d], other_ref[:, d]).astype(f32)
            rounded = total.astype(bf16)
            v = (start[:, :value_width] + product(rounded, mix_ref[m])) * r
            low = start[:, value_width : value_width + rank]
            low = low + product_bt(rounded, small_ref[m, :rank])
            v_ref[m] = v
            lows.append((low * r).astype(bf16))
            before.append(rounded)
            inverse.append(r)
            total = total + v
        for copy in copies:
            copy.wait()
        direction = tail[:, 2 * value_width : 3 * value_width].astype(f32)
        grown = jnp.zeros((tokens, rows), f32)
        writes = []
        for m in reversed(range(sections)):
            r = inverse[m]
            rounded = direction.astype(bf16)
            mean = jnp.sum(rounded.astype(f32) * v_ref[m], axis=1, keepdims=True) / width
            q = mean * r * r
            scaled = (direction * r).astype(bf16)
            low_grad = adapter_scale * product_bt(rounded, small_ref[m, rank : 2 * rank]) * r
            grad_ref[m, :, rows:] = (adapter_scale * product_at(lows[m], rounded)).astype(bf16)
            earlier = before[m].astype(f32)
            spread = jnp.zeros((tokens, HEAD), f32)
            for k in range(KV_HEADS):
                spread = spread + jnp.where(head == k, earlier[:, k * HEAD : (k + 1) * HEAD], 0.0)
            hidden = hx + jnp.concatenate([spread] * groups, axis=1)
            grad_ref[m, :, :rows] = product_at(
                low_grad.astype(bf16), hidden.astype(bf16)
            ).astype(bf16)
            grown = grown + product_bt(scaled, w_ref[m]) - hidden * q
            out = grown.astype(bf16).reshape(2, chips, quarter, rows)
            for e in range(2):
                for z in range(chips):
                    out_ref[m, 2 * z + (core ^ e)] = out[e, z]
            writes.append(pltpu.make_async_copy(out_ref.at[m], out_hbm.at[m], sems.at[4, m]))
            writes[-1].start()
            direction = direction + product_bt(scaled, mix_ref[m]) - (ch + GROUP * earlier) * q
        for d in range(sections):
            writes.append(
                pltpu.make_async_copy(grad_ref.at[me ^ d], grad_refs[d], sems.at[5, d])
            )
            writes[-1].start()
        for copy in writes:
            copy.wait()

    vmem = pl.BlockSpec(memory_space=pltpu.VMEM)
    anywhere = pl.BlockSpec(memory_space=pl.ANY)
    flat = [piece for pair in weights for piece in pair]
    grad_width = rows + value_width
    outs = pl.pallas_call(
        kernel,
        in_specs=[pl.BlockSpec(memory_space=pltpu.SMEM)]
        + [vmem] * 6
        + [anywhere] * (4 * sections),
        out_shape=[jax.ShapeDtypeStruct((sections, 2 * chips, quarter, rows), bf16)]
        + [jax.ShapeDtypeStruct((rank, grad_width), bf16)] * sections,
        out_specs=[pl.BlockSpec(memory_space=pltpu.HBM)] * (1 + sections),
        scratch_shapes=[
            pltpu.VMEM((sections, 2 * chips, quarter, rows), bf16),
            pltpu.VMEM((sections, tokens, value_width), f32),
            pltpu.VMEM((sections, value_width, value_width), bf16),
            pltpu.VMEM((sections, 2 * rank, value_width), bf16),
            pltpu.VMEM((sections, rows, value_width), bf16),
            pltpu.VMEM((sections, rank, grad_width), bf16),
            pltpu.SemaphoreType.DMA((6, sections)),
        ],
        compiler_params=pltpu.CompilerParams(vmem_limit_bytes=(60 * 1024 * 1024) - (1344 << 10)),
        name="chain",
    )(index, sums, other_sums, own, given, *tails, *mixings, *smalls, *flat)
    return outs[0], outs[1:]


def placed(moved, cotangent):
    sections, devices, quarter, rows = moved.shape
    count, width = cotangent.shape
    halves = 1
    each = devices // halves

    def kernel(m_ref, c_ref, out_ref):
        for j in range(each):
            at = slice(j * rows, (j + 1) * rows)
            out_ref[0, :, at] = (c_ref[:, at].astype(f32) + m_ref[0, j].astype(f32)).astype(bf16)

    return pl.pallas_call(
        kernel,
        grid=(sections, halves),
        in_specs=[
            pl.BlockSpec((1, each, quarter, rows), lambda i, h: (i, h, 0, 0)),
            pl.BlockSpec((quarter, each * rows), lambda i, h: (i, h)),
        ],
        out_specs=pl.BlockSpec((1, quarter, each * rows), lambda i, h: (0, i, h)),
        out_shape=jax.ShapeDtypeStruct((1, count, width), bf16),
        compiler_params=room(8),
        name="placed",
    )(moved, cotangent)


def layers(
    codes,
    scale_codes,
    second_scales,
    gains,
    down_adapter,
    up_projection_weight,
    hidden_in,
    cotangent,
):
    fsdp = ("chip", "core")
    s = lax.axis_index("section")
    j = lax.axis_index(fsdp)
    sections = lax.axis_size("section")
    chips = lax.axis_size("chip")
    devices = lax.axis_size(fsdp)
    count, width = hidden_in.shape
    quarter = count // sections
    rows, value_width = codes.shape[1], codes.shape[2]
    index = jnp.stack([s, j, j * rows // (GROUP * HEAD)]).astype(jnp.int32)
    scale_codes = jnp.swapaxes(scale_codes, 1, 2)
    down = jnp.swapaxes(down_adapter, 1, 2)
    up = jnp.swapaxes(up_projection_weight, 1, 2)

    first, second, block = effective_rows(
        index, codes, scale_codes, second_scales, gains, down, up
    )
    weights = forwarded((first, second), "section")

    own, tail = hidden_parts(index, hidden_in, cotangent, block, quarter, rows, chips)
    own = exchange(own, "chip")
    given = swap(own[:, :, rows:], "core", 1)
    tails = [tail]
    for d in range(1, chips):
        tails.append(swap(tail, "chip", d))
    tail = in_chip_order(index, tails)
    tails = (tail, swap(tail, "core", 1))

    smalls = list(low_rank_parts(index, hidden_in, gains, down, up, quarter, sections))
    for d in range(1, sections):
        smalls[d] = swap(smalls[d], "section", d)

    mixing = mixing_matrix(index, *tails, quarter, SPREAD // rows)
    mixings = [mixing]
    for d in range(1, sections):
        mixings.append(swap(mixing, "section", d))

    mine, other = partial_products(own, given, weights, rows)
    other = swap(other, "core", 1)
    pieces = sum_cores(mine, other)
    pieces = exchange(pieces, "chip")
    sums = sum_chips(pieces, smalls)
    sums = exchange(sums, "chip")
    other_sums = swap(sums, "core", 1)

    grown, grads = chain(
        index, sums, other_sums, own, given, tails, mixings, smalls, weights, rows, width
    )

    gradient = grads[0].astype(f32)
    for d in range(1, sections):
        gradient = gradient + swap(grads[d], "section", d).astype(f32)
    per = value_width // devices
    gain_here = lax.dynamic_slice_in_dim(gains[0].astype(f32), j * rows, rows)
    down_grad = (gradient[:, :rows] * gain_here[None, :]).T
    up_grad = lax.dynamic_slice_in_dim(gradient[:, rows:], j * per, per, 1).T

    moved = grown.reshape(sections * devices, quarter, rows)
    moved = exchange(moved, ("section", "chip", "core"))
    input_grad = placed(moved.reshape(sections, devices, quarter, rows), cotangent)
    return (input_grad, down_grad[None], up_grad[None])


def solution(mesh):
    sections, devices = mesh.devices.shape
    split = jax.sharding.Mesh(
        mesh.devices.reshape(sections, devices // 2, 2), ("section", "chip", "core")
    )
    fsdp = ("chip", "core")
    return jax.shard_map(
        layers,
        mesh=split,
        in_specs=(
            P("section", fsdp, None),
            P("section", fsdp, None),
            P("section", fsdp),
            P("section", None),
            P("section", None, None),
            P("section", None, None),
            P(fsdp, None),
            P(fsdp, None),
        ),
        out_specs=(
            P("section", fsdp, None),
            P("section", fsdp, None),
            P("section", fsdp, None),
        ),
        check_vma=False,
    )
```
